256 devices in a mesh: sx: 8 (over y, core), sy: 8 (over z), af: 4 (over x).
Axes of the slice: x: 4, y: 4, z: 8, core: 2. Of those that a mesh axis runs over, the one named last changes fastest.
Arguments:
- sky_maps: float32 [256, 256, 1024], P('sx', 'sy', 'af'), may hold values from -16 to 25
- validity: int32 [256, 256], P('sx', 'sy'), may hold values 0 or 1
- row_taps: float32 [1024, 65], P('af'), may hold values from -0.75 to 0.75
- column_taps: float32 [1024, 65], P('af'), may hold values from -0.75 to 0.75
- init_loadings: float32 [1024, 32], P('af'), may hold values from -0.1875 to 0.1875
Outputs:
- cleaned_maps: float32 [256, 256, 1024], P('sx', 'sy', 'af')
- loadings: float32 [1024, 32], P('af')
- noise_var: float32 [], replicated
The draws below stay inside these ranges and needn't reach their ends.
All inputs are finite; a program needn't handle non-finite values. No bound on the sum of `validity` on one device may be relied on, other than what follows from the above.
Results may differ from the reference program's by a relative error of at most 0.0003.
Values sent between devices are 32-bit elements; how exact they have to be, the bound alone decides.
No kernel may reach another device: no remote copies, remote signals or barrier semaphores. Data moves between devices by JAX's collectives and lax.ppermute only.
A program may use at most 128 MiB of HBM per device.

```python
import math
import jax
import jax.numpy as jnp
from jax import lax

FREQS = 1024
COMPONENTS = 32
TAPS = 65
ITERS = 4
HALO = 32
NR = 256
NC = 256
NPIX = 65536


def draw_sky_maps(key, part):
    subkeys = jax.random.split(key, 5)
    pixel_shape = (NR, NC, 1)
    row_place = jnp.arange(NR, dtype=jnp.float32)[:, None, None]
    frequency = jnp.arange(FREQS, dtype=jnp.float32)[None, None, :]
    log_ratio = jnp.log(1.0 + frequency / FREQS)
    spread = 0.7
    noise_part = jnp.clip(jax.random.normal(subkeys[0], (NR, NC, FREQS), jnp.float32), -5.0, 5.0)
    gradient = jnp.exp(jnp.log(3.0) * row_place / NR)
    first_amp = jnp.exp(jax.random.uniform(subkeys[1], pixel_shape, jnp.float32, -spread, spread))
    first_index = jax.random.uniform(subkeys[2], pixel_shape, jnp.float32, 2.4, 3.0)
    second_amp = jnp.exp(jax.random.uniform(subkeys[3], pixel_shape, jnp.float32, -spread, spread))
    second_index = jax.random.uniform(subkeys[4], pixel_shape, jnp.float32, 1.9, 2.2)
    foreground = first_amp * jnp.exp(-first_index * log_ratio) + 0.6 * second_amp * jnp.exp(-second_index * log_ratio)
    return (gradient * (foreground + noise_part)).astype(jnp.float32)


def touch_ends(entries, rng, low, top_value):
    longest = entries.shape.index(max(entries.shape))
    spots = []
    for shift in (0, 1):
        where = [jax.random.randint(jax.random.fold_in(rng, axis), (), 0, length) for axis, length in enumerate(entries.shape)]
        where[longest] = (where[longest] + shift) % entries.shape[longest]
        spots.append(tuple(where))
    return entries.at[spots[0]].set(low).at[spots[1]].set(top_value)


def shard_levels(rng, shape, cuts, least, top_value):
    gain, own = 1.0, jax.random.fold_in(rng, 6)
    for dim, blocks in cuts:
        steps = jnp.exp(jax.random.uniform(jax.random.fold_in(own, dim), (blocks,), jnp.float32, least / len(cuts), top_value / len(cuts)))
        gain = gain * jnp.repeat(steps, shape[dim] // blocks).reshape([-1 if axis == dim else 1 for axis in range(len(shape))])
    return gain


def gaussian(own_key, shape, deviation, reach, cuts=(), kind=jnp.bfloat16):
    values = jax.random.normal(own_key, shape, jnp.float32) * deviation
    if len(cuts) > 0:
        values = shard_levels(own_key, shape, cuts, -0.22, 0.18) * values
    return jnp.clip(values, min=-reach, max=reach).astype(kind)


def setup_inputs(seed: int = 0) -> dict:
    key_list = jax.random.split(jax.random.key(seed), 6)
    return {
        "sky_maps": draw_sky_maps(jax.random.fold_in(key_list[5], 71), 0),
        "validity": touch_ends((jax.random.randint(key_list[1], (NR, NC), 0, 8) < 7).astype(jnp.int32), jax.random.fold_in(key_list[1], 1), 0, 1),
        "row_taps": gaussian(key_list[2], (FREQS, TAPS), TAPS ** -0.5, 0.75, ((0, 4),), jnp.float32),
        "column_taps": gaussian(key_list[3], (FREQS, TAPS), TAPS ** -0.5, 0.75, ((0, 4),), jnp.float32),
        "init_loadings": gaussian(key_list[4], (FREQS, COMPONENTS), FREQS ** -0.5, 0.1875, ((0, 4),), jnp.float32),
    }


HIGHEST_PRECISION = lax.Precision.HIGHEST

def inverse_spd(matrix):
    identity = jnp.eye(matrix.shape[0], dtype=matrix.dtype)
    factor = jnp.linalg.cholesky(matrix)
    lower_inverse = lax.linalg.triangular_solve(factor, identity, left_side=True, lower=True)
    return jnp.dot(lower_inverse.T, lower_inverse, precision=HIGHEST_PRECISION)

def reference(sky_maps, validity, row_taps, column_taps, init_loadings):
    masked = sky_maps * validity.astype(jnp.float32)[:, :, None]
    block_size = math.gcd(FREQS, 16)

    def beam_block(first_freq):
        slab_part = lax.dynamic_slice_in_dim(masked, first_freq, block_size, 2)
        row_block = lax.dynamic_slice_in_dim(row_taps, first_freq, block_size, 0)
        column_block = lax.dynamic_slice_in_dim(column_taps, first_freq, block_size, 0)
        padded = jnp.pad(slab_part, ((HALO, HALO), (0, 0), (0, 0)))
        smoothed = jnp.zeros_like(slab_part)
        for tap_place in range(TAPS):
            smoothed = smoothed + row_block[:, tap_place] * padded[tap_place:tap_place + NR]
        padded = jnp.pad(smoothed, ((0, 0), (HALO, HALO), (0, 0)))
        beamed = jnp.zeros_like(slab_part)
        for tap_place in range(TAPS):
            beamed = beamed + column_block[:, tap_place] * padded[:, tap_place:tap_place + NC]
        return beamed
    starts = jnp.arange(FREQS // block_size, dtype=jnp.int32) * block_size
    stacked = lax.map(beam_block, starts)
    spectra = jnp.moveaxis(stacked, 0, 2).reshape(NPIX, FREQS)
    total_power = jnp.sum(spectra * spectra)
    identity = jnp.eye(COMPONENTS, dtype=jnp.float32)
    loadings = init_loadings
    noise_var = jnp.float32(1.0)
    for iteration in range(ITERS):
        gram_matrix = jnp.dot(loadings.T, loadings, precision=HIGHEST_PRECISION)
        inverse = inverse_spd(gram_matrix + noise_var * identity)
        latent = jnp.dot(spectra, jnp.dot(loadings, inverse, precision=HIGHEST_PRECISION), precision=HIGHEST_PRECISION)
        cross_moment = jnp.dot(spectra.T, latent, precision=HIGHEST_PRECISION)
        second = jnp.dot(latent.T, latent, precision=HIGHEST_PRECISION)
        scaled = NPIX * noise_var * inverse + second
        updated = jnp.dot(cross_moment, inverse_spd(scaled), precision=HIGHEST_PRECISION)
        new_gram = jnp.dot(updated.T, updated, precision=HIGHEST_PRECISION)
        noise_var = (total_power - 2.0 * jnp.sum(updated * cross_moment) + jnp.sum(scaled * new_gram)) / (NPIX * FREQS)
        loadings = updated
    gram_matrix = jnp.dot(loadings.T, loadings, precision=HIGHEST_PRECISION)
    inverse = inverse_spd(gram_matrix + noise_var * identity)
    latent = jnp.dot(spectra, jnp.dot(loadings, inverse, precision=HIGHEST_PRECISION), precision=HIGHEST_PRECISION)
    cleaned = spectra - jnp.dot(latent, loadings.T, precision=HIGHEST_PRECISION)
    return (cleaned.reshape(NR, NC, FREQS), loadings, noise_var)
```

```python
import functools

import jax
import jax.numpy as jnp
from jax import lax
from jax.experimental import pallas as pl
from jax.experimental.pallas import tpu as pltpu
from jax.sharding import PartitionSpec as P

ITERS = 4
HI = lax.Precision.HIGHEST
VM = pltpu.VMEM
INTERPRET = False


def call(kernel, **kw):
    return pl.pallas_call(kernel, interpret=INTERPRET, **kw)


def contract(left, right, dims):
    return lax.dot_general(
        left, right, (dims, ((), ())), precision=HI, preferred_element_type=jnp.float32
    )


def beam_kernel(low, own, high, taps, out):
    length = own.shape[0]
    count = taps.shape[0]
    refs = (low, own, high)
    for block in range(length // 8):
        acc = [None] * 8
        held = {}
        for k in range(count + 7):
            row = block * 8 + k
            value = refs[row // length][row % length]
            if k < count:
                held[k] = taps[k]
            for j in range(8):
                t = k - j
                if 0 <= t < count:
                    term = held[t] * value
                    acc[j] = term if acc[j] is None else acc[j] + term
        out[:, block * 8 : block * 8 + 8, :] = jnp.swapaxes(jnp.stack(acc), 0, 1)


def beam(low, own, high, taps):
    a, b, f = own.shape
    assert taps.shape[0] == 2 * a + 1
    spec = pl.BlockSpec((a, 8, f), lambda j: (0, j, 0))
    return call(
        beam_kernel,
        grid=(b // 8,),
        in_specs=[spec, spec, spec, pl.BlockSpec(taps.shape, lambda j: (0, 0, 0))],
        out_specs=pl.BlockSpec((8, a, f), lambda j: (j, 0, 0)),
        out_shape=jax.ShapeDtypeStruct((b, a, f), jnp.float32),
        name="beam",
    )(low, own, high, taps)


def row_block(place, c, k, parts):
    return lax.rem(place[0] + c, 2) * parts + lax.rem(place[1] + k, parts)


def moment_kernel(place, even, odd, out):
    parts = even.shape[0]
    blocks = 2 * parts
    c, k = pl.program_id(0), pl.program_id(1)
    i = row_block(place, c, k, parts)

    def column(b):
        half = lax.div(b, 2)
        return jnp.where(lax.rem(b, 2) == 0, even[half], odd[half])

    cols = [column(lax.rem(i + j, blocks)) for j in range(parts + 1)]
    out[0, 0] = contract(cols[0], jnp.concatenate(cols, axis=1), ((0,), (0,)))


def moments(place, even, odd):
    parts, pixels, width = even.shape
    full = pl.BlockSpec(even.shape, lambda c, k, place: (0, 0, 0))
    return call(
        moment_kernel,
        grid_spec=pltpu.PrefetchScalarGridSpec(
            num_scalar_prefetch=1,
            grid=(2, parts),
            in_specs=[full, full],
            out_specs=pl.BlockSpec(
                (1, 1, width, width * (parts + 1)), lambda c, k, place: (c, k, 0, 0)
            ),
        ),
        out_shape=jax.ShapeDtypeStruct((2, parts, width, width * (parts + 1)), jnp.float32),
        name="moments",
    )(place, even, odd)


def inverse_spd(matrix):
    n = matrix.shape[0]
    rows = lax.broadcasted_iota(jnp.int32, (n, n), 0)
    lanes = lax.broadcasted_iota(jnp.int32, (n, n), 1)
    lane = lax.broadcasted_iota(jnp.int32, (1, n), 1)
    for k in range(n):
        pivot = 1.0 / matrix[k : k + 1, k : k + 1]
        row = jnp.where(lane == k, 1.0, matrix[k : k + 1, :]) * pivot
        col = matrix[:, k : k + 1]
        matrix = jnp.where(rows == k, row, jnp.where(lanes == k, 0.0, matrix) - col * row)
    return matrix


def total(x):
    return jnp.sum(jnp.sum(x, axis=1, keepdims=True), axis=0, keepdims=True)


def fit_kernel(pixel_total, place, mine, other, start, even, odd, load_out, noise_out, lat_out, full):
    parts, width, span = mine.shape
    blocks = 2 * parts
    freqs = blocks * width
    n = start.shape[0]
    eye_block = (
        lax.broadcasted_iota(jnp.int32, (width, width), 0)
        == lax.broadcasted_iota(jnp.int32, (width, width), 1)
    )
    power = jnp.zeros((1, 1), jnp.float32)
    for c, ref in enumerate((mine, other)):
        for k in range(parts):
            i = row_block(place, c, parts - k, parts)
            for j in range(parts + 1):
                block = ref[k, :, j * width : (j + 1) * width]
                at_row = pl.multiple_of(i * width, width)
                at_col = pl.multiple_of(lax.rem(i + j, blocks) * width, width)
                full[pl.ds(at_row, width), pl.ds(at_col, width)] = block
                if j == 0:
                    power = power + total(jnp.where(eye_block, block, 0.0))
                elif j < parts:
                    full[pl.ds(at_col, width), pl.ds(at_row, width)] = block.T
    eye = (
        lax.broadcasted_iota(jnp.int32, (n, n), 0) == lax.broadcasted_iota(jnp.int32, (n, n), 1)
    ).astype(jnp.float32)

    def weights(loads, gram, noise):
        inverse = inverse_spd(gram + noise * eye)
        return inverse, contract(inverse, loads, ((1,), (0,)))

    def step(_, state):
        loads, gram, noise = state
        inverse, weight = weights(loads, gram, noise)
        cross = contract(weight, full[...], ((1,), (0,)))
        second = contract(cross, weight, ((1,), (1,)))
        scaled = pixel_total * noise * inverse + second
        updated = contract(inverse_spd(scaled), cross, ((1,), (0,)))
        new_gram = contract(updated, updated, ((1,), (1,)))
        noise = (power - 2.0 * total(updated * cross) + total(scaled * new_gram)) / (
            pixel_total * freqs
        )
        return updated, new_gram, noise

    loads = start[...]
    state = (loads, contract(loads, loads, ((1,), (1,))), jnp.ones((1, 1), jnp.float32))
    loads, gram, noise = lax.fori_loop(0, ITERS, step, state)
    load_out[...] = loads
    noise_out[...] = noise
    weight = weights(loads, gram, noise)[1]
    latent = None
    for b in range(blocks):
        ref = (even, odd)[b % 2]
        term = contract(weight[:, b * width : (b + 1) * width], ref[b // 2], ((1,), (1,)))
        latent = term if latent is None else latent + term
    lat_out[...] = latent


def fit(place, mine, other, start, even, odd, pixel_total):
    n, freqs = start.shape
    vmem = pl.BlockSpec(memory_space=VM)
    return call(
        functools.partial(fit_kernel, pixel_total),
        in_specs=[pl.BlockSpec(memory_space=pltpu.SMEM)] + [vmem] * 5,
        out_specs=[vmem] * 3,
        out_shape=[
            jax.ShapeDtypeStruct((n, freqs), jnp.float32),
            jax.ShapeDtypeStruct((1, 1), jnp.float32),
            jax.ShapeDtypeStruct((n, even.shape[1]), jnp.float32),
        ],
        scratch_shapes=[VM((freqs, freqs), jnp.float32)],
        name="fit",
    )(place, mine, other, start, even, odd)


def clean_kernel(place, first, second, latents, loads, out):
    width = first.shape[1]
    for half, ref in enumerate((first, second)):
        out[:, half * width : (half + 1) * width] = ref[...] - contract(
            latents[0], loads[:, half * width : (half + 1) * width], ((0,), (0,))
        )


def clean(place, first, second, latents, loads):
    pixels, width = first.shape
    parts, n, rows = latents.shape

    def block(k, place):
        return (lax.rem(place[1] + parts - k, parts), 0)

    spec = pl.BlockSpec((rows, width), block)
    return call(
        clean_kernel,
        grid_spec=pltpu.PrefetchScalarGridSpec(
            num_scalar_prefetch=1,
            grid=(parts,),
            in_specs=[
                spec,
                spec,
                pl.BlockSpec((1, n, rows), lambda k, place: (k, 0, 0)),
                pl.BlockSpec(loads.shape, lambda k, place: (0, 0)),
            ],
            out_specs=pl.BlockSpec((rows, 2 * width), block),
        ),
        out_shape=jax.ShapeDtypeStruct((pixels, 2 * width), jnp.float32),
        name="clean",
    )(place, first, second, latents, loads)


def body(sky_maps, validity, row_taps, column_taps, init_loadings):
    rows_here, cols_here, freqs_here = sky_maps.shape
    sx, sy, af = (lax.axis_size(a) for a in ("sx", "sy", "af"))
    width = freqs_here // 2
    n = init_loadings.shape[1]
    pixels_here = rows_here * cols_here
    af_index = lax.axis_index("af")
    place = jnp.stack([lax.rem(lax.axis_index("sx"), 2), af_index]).astype(jnp.int32)
    mask = validity.astype(jnp.float32)[:, :, None]

    def halos(block, axis, count):
        low = lax.ppermute(block, axis, [(i, i + 1) for i in range(count - 1)])
        high = lax.ppermute(block, axis, [(i + 1, i) for i in range(count - 1)])
        return low, high

    def spread(taps, half):
        table = taps[half * width : (half + 1) * width].T[:, None, :]
        return jnp.broadcast_to(table, (table.shape[0], 8, width))

    def shifted(block, k):
        return lax.ppermute(block, "af", [(i, (i + k) % af) for i in range(af)])

    start_block = init_loadings.T
    start_all = lax.all_gather(start_block, "af", axis=1, tiled=True)

    beamed, traded = [], []
    masked = [sky_maps[:, :, h * width : (h + 1) * width] * mask for h in range(2)]
    around = [halos(m, "sx", sx) for m in masked]
    for h in range(2):
        smoothed = beam(around[h][0], masked[h], around[h][1], spread(row_taps, h))
        low, high = halos(smoothed, "sy", sy)
        spectra = beam(low, smoothed, high, spread(column_taps, h)).reshape(pixels_here, width)
        beamed.append(spectra)
        traded.append(
            lax.all_to_all(spectra.reshape(af, pixels_here // af, width), "af", 0, 0)
        )
    even, odd = traded

    partial = moments(place, even, odd)
    partial = partial[0] + lax.ppermute(partial[1], "sx", [(i, i ^ 1) for i in range(sx)])
    piece = partial[0]
    for k in range(1, af):
        piece = piece + shifted(partial[k], k)
    ranks = sx * sy // 2
    groups = [
        [s * sy + t for s in range(c, sx, 2) for t in range(sy)] for c in range(2)
    ]
    shape = piece.shape
    pieces = piece.reshape(ranks, -1, shape[1])
    pieces = lax.all_to_all(pieces, ("sx", "sy"), 0, 0, axis_index_groups=groups)
    owned = jnp.sum(pieces, axis=0)
    pieces = lax.all_to_all(
        jnp.broadcast_to(owned[None], pieces.shape), ("sx", "sy"), 0, 0, axis_index_groups=groups
    )
    piece = pieces.reshape(shape)
    mine = jnp.stack([piece] + [shifted(piece, k) for k in range(1, af)])
    other = lax.ppermute(mine, "sx", [(i, i ^ 1) for i in range(sx)])

    loadings, noise, latent = fit(
        place, mine, other, start_all, even, odd, float(pixels_here * sx * sy)
    )
    latents = jnp.stack([latent] + [shifted(latent, k) for k in range(1, af)])
    loads_here = lax.dynamic_slice_in_dim(loadings, af_index * freqs_here, freqs_here, 1)
    cleaned = clean(place, beamed[0], beamed[1], latents, loads_here)
    return (
        cleaned.reshape(rows_here, cols_here, freqs_here),
        loads_here.T,
        noise.reshape(()),
    )


def solution(mesh):
    placed = (P("sx", "sy", "af"), P("sx", "sy"), P("af", None), P("af", None), P("af", None))
    return jax.shard_map(
        body,
        mesh=mesh,
        in_specs=placed,
        out_specs=(P("sx", "sy", "af"), P("af", None), P()),
        check_vma=False,
    )
```

```python
import functools

import jax
import jax.numpy as jnp
from jax import lax
from jax.experimental import pallas as pl
from jax.experimental.pallas import tpu as pltpu
from jax.sharding import PartitionSpec as P

ITERS = 4
HI = lax.Precision.HIGHEST
VM = pltpu.VMEM
INTERPRET = False
LIMIT = 32 << 20


def call(kernel, out_shapes, *args, name, scratch=(), dtypes=None):
    dtypes = dtypes or [jnp.float32] * len(out_shapes)
    fast = pl.BlockSpec(memory_space=VM)
    specs = [
        pl.BlockSpec(memory_space=pltpu.SMEM) if x.dtype == jnp.int32 else fast for x in args
    ]
    if INTERPRET:
        outs = [jax.ShapeDtypeStruct(s, d) for s, d in zip(out_shapes, dtypes)]
    else:
        outs = [VM(s, d) for s, d in zip(out_shapes, dtypes)]
        args = [
            x if x.dtype == jnp.int32 else pltpu.with_memory_space_constraint(x, VM) for x in args
        ]
    return pl.pallas_call(
        kernel,
        out_shape=outs,
        in_specs=specs,
        out_specs=[fast] * len(outs),
        scratch_shapes=list(scratch),
        compiler_params=pltpu.CompilerParams(vmem_limit_bytes=LIMIT),
        interpret=INTERPRET,
        name=name,
    )(*args)


def contract(left, right, dims):
    return lax.dot_general(
        left, right, (dims, ((), ())), precision=HI, preferred_element_type=jnp.float32
    )


def split3(x):
    hi = x.astype(jnp.bfloat16)
    rest = x - hi.astype(jnp.float32)
    mid = rest.astype(jnp.bfloat16)
    low = (rest - mid.astype(jnp.float32)).astype(jnp.bfloat16)
    return hi, mid, low


def thin(left, right, dims):
    (ld,), (rd,) = dims
    lh, lm, ll = split3(left)
    rh, rm, rl = split3(right)
    a = jnp.concatenate([ll, lm, lh, lm, lh, lh], axis=ld)
    b = jnp.concatenate([rh, rm, rl, rh, rm, rh], axis=rd)
    return lax.dot_general(a, b, (dims, ((), ())), preferred_element_type=jnp.float32)


def beam_kernel(half, low, own, high, taps, *rest):
    out = rest[-1]
    length, wide, width = own.shape
    count = taps.shape[0]
    refs = (low, own, high)
    lanes = slice(half * width, (half + 1) * width)

    def strip(j, _):
        at = pl.ds(pl.multiple_of(j * 8, 8), 8)
        for block in range(length // 8):
            acc = [None] * 8
            held = {}
            for k in range(count + 7):
                row = block * 8 + k
                value = refs[row // length][row % length, at, :]
                if k < count:
                    held[k] = jnp.broadcast_to(taps[k : k + 1, lanes], value.shape)
                for i in range(8):
                    t = k - i
                    if 0 <= t < count:
                        term = held[t] * value
                        acc[i] = term if acc[i] is None else acc[i] + term
            out[j, 0:8, block * 8 : block * 8 + 8, :] = jnp.swapaxes(jnp.stack(acc), 0, 1)
        if len(rest) == 2:
            for e in range(out.shape[1] - 8):
                out[j, 8 + e] = rest[0][e * length : (e + 1) * length, lanes]

    lax.fori_loop(0, wide // 8, strip, None)


def beam(low, own, high, taps, half, loads=None):
    a, b, f = own.shape
    assert taps.shape[0] == 2 * a + 1
    more = [] if loads is None else [loads]
    extra = 0 if loads is None else loads.shape[0] // a
    shape = (b // 8, 8 + extra, a, f)
    kernel = functools.partial(beam_kernel, half)
    return call(kernel, [shape], low, own, high, taps, *more, name="beam")[0]


def row_block(place, c, k, parts):
    return lax.rem(place[0] + c, 2) * parts + lax.rem(place[1] + k, parts)


def moment_kernel(c, pixels, place, *refs):
    if len(refs) == 5:
        even, odd, out, hi, lo = refs
        parts = even.shape[0]
        for b in range(2 * parts):
            value = (even, odd)[b % 2][b // 2, 0:pixels]
            top = value.astype(jnp.bfloat16)
            hi[b] = top
            lo[b] = (value - top.astype(jnp.float32)).astype(jnp.bfloat16)
    else:
        hi, lo, out = refs
        parts = hi.shape[0] // 2
    blocks = 2 * parts
    for k in range(parts):
        i = row_block(place, c, k, parts)
        at = [lax.rem(i + j, blocks) for j in range(parts + 1)]
        left = jnp.concatenate([lo[i], hi[i], hi[i]], axis=0)
        high = jnp.concatenate([hi[b] for b in at], axis=1)
        low = jnp.concatenate([lo[b] for b in at], axis=1)
        right = jnp.concatenate([high, low, high], axis=0)
        out[k] = lax.dot_general(
            left, right, (((0,), (0,)), ((), ())), preferred_element_type=jnp.float32
        )


def moments(place, even, odd, pixels):
    parts, _, width = even.shape
    shape = (parts, width, width * (parts + 1))
    halves = (2 * parts, pixels, width)
    half = jnp.bfloat16
    theirs, hi, lo = call(
        functools.partial(moment_kernel, 1, pixels), [shape, halves, halves], place, even, odd,
        name="moments", dtypes=[jnp.float32, half, half],
    )
    ours = call(functools.partial(moment_kernel, 0, pixels), [shape], place, hi, lo, name="moments")
    return theirs, ours[0], hi, lo


def inverse_spd(matrix):
    n = matrix.shape[0]
    lane = lax.broadcasted_iota(jnp.int32, (8, n), 1)
    row = lax.broadcasted_iota(jnp.int32, (8, n), 0)
    unit = 1.0 / jnp.broadcast_to(matrix[0:1, 0:1], (8, n))
    tiles = [matrix[i : i + 8] * unit for i in range(0, n, 8)]
    for k in range(0, n, 2):
        at, r = divmod(k, 8)

        def every(tile, s):
            return jnp.broadcast_to(tile[s : s + 1], (8, n))

        left = [jnp.broadcast_to(t[:, k : k + 1], (8, n)) for t in tiles]
        right = [jnp.broadcast_to(t[:, k + 1 : k + 2], (8, n)) for t in tiles]
        a, b = every(left[at], r), every(right[at], r)
        c, d = every(left[at], r + 1), every(right[at], r + 1)
        pivot = 1.0 / (a * d - b * c)
        inside = (lane == k) | (lane == k + 1)
        top = jnp.where(inside, (lane == k).astype(jnp.float32), every(tiles[at], r))
        low = jnp.where(inside, (lane == k + 1).astype(jnp.float32), every(tiles[at], r + 1))
        first = (d * top - b * low) * pivot
        second = (a * low - c * top) * pivot
        tiles = [
            jnp.where(inside, 0.0, t) - x * first - y * second
            for t, x, y in zip(tiles, left, right)
        ]
        tiles[at] = jnp.where(row == r, first, jnp.where(row == r + 1, second, tiles[at]))
    return jnp.concatenate([t * unit for t in tiles], axis=0)


def total(x):
    return jnp.sum(jnp.sum(x, axis=1, keepdims=True), axis=0, keepdims=True)


def identity(n):
    return lax.broadcasted_iota(jnp.int32, (n, n), 0) == lax.broadcasted_iota(jnp.int32, (n, n), 1)


def weights(loads, gram, noise):
    inverse = inverse_spd(gram + jnp.where(identity(gram.shape[0]), noise, 0.0))
    return inverse, thin(inverse, loads, ((1,), (0,)))


def first_kernel(even, odd, inverse_out, weight_out):
    n = weight_out.shape[0]
    rows = even.shape[1]
    loads = jnp.concatenate(
        [ref[b, rows - n : rows] for b in range(even.shape[0]) for ref in (even, odd)], axis=1
    )
    gram = contract(loads, loads, ((1,), (1,)))
    inverse_out[...], weight_out[...] = weights(loads, gram, jnp.ones((1, 1), jnp.float32))


def first_weights(even, odd, n):
    parts, _, width = even.shape
    return call(first_kernel, [(n, n), (n, 2 * parts * width)], even, odd, name="first")


def cross_of(weight, hi, mid, low):
    n = weight.shape[0]
    stacked = jnp.concatenate(split3(weight), axis=0)

    def product(count, ref):
        return jnp.dot(stacked[: count * n], ref[...], preferred_element_type=jnp.float32)

    top, middle, last = product(3, hi), product(2, mid), product(1, low)
    small = top[2 * n :] + middle[n:] + last
    return top[:n] + (top[n : 2 * n] + middle[:n] + small)


def fit_kernel(pixel_total, parts, place, *refs):
    slots = refs[: 2 * parts]
    inverse0, weight0, map_hi, map_lo = refs[2 * parts : 2 * parts + 4]
    block_out, noise_out, lat_out, hi, mid, low, held = refs[2 * parts + 4 :]
    width = slots[0].shape[0]
    blocks = 2 * parts
    freqs = blocks * width
    n = weight0.shape[0]
    diagonal = identity(width)
    power = jnp.zeros((width, width), jnp.float32)
    for s, ref in enumerate(slots):
        i = row_block(place, s // parts, parts - s % parts, parts)
        for j in range(parts + 1):
            block = ref[:, j * width : (j + 1) * width]
            at_row = pl.multiple_of(i * width, width)
            at_col = pl.multiple_of(lax.rem(i + j, blocks) * width, width)
            for dest, value in zip((hi, mid, low), split3(block)):
                dest[pl.ds(at_row, width), pl.ds(at_col, width)] = value
            if j == 0:
                power = power + jnp.where(diagonal, block, 0.0)
            elif j < parts:
                for dest, value in zip((hi, mid, low), split3(block.T)):
                    dest[pl.ds(at_col, width), pl.ds(at_row, width)] = value
    power = total(power)

    def step(_, state):
        inverse, weight, noise = state
        cross = cross_of(weight, hi, mid, low)
        second = contract(cross, weight, ((1,), (1,)))
        scaled = pixel_total * noise * inverse + second
        updated = thin(inverse_spd(scaled), cross, ((1,), (0,)))
        held[...] = updated
        gram = contract(updated, updated, ((1,), (1,)))
        noise = (power - 2.0 * total(updated * cross) + total(scaled * gram)) / (
            pixel_total * freqs
        )
        return (*weights(updated, gram, noise), noise)

    state = (inverse0[...], weight0[...], jnp.ones((1, 1), jnp.float32))
    _, weight, noise = lax.fori_loop(0, ITERS, step, state)
    noise_out[...] = noise
    here = block_out.shape[1]
    block_out[...] = held[:, pl.ds(pl.multiple_of(place[1] * here, here), here)]
    whigh, wlow, _ = split3(weight)
    pair = jnp.concatenate([whigh, wlow], axis=0)
    latent = None
    for b in range(blocks):
        lanes = slice(b * width, (b + 1) * width)
        dims = (((1,), (1,)), ((), ()))
        both = lax.dot_general(
            pair[:, lanes], map_hi[b], dims, preferred_element_type=jnp.float32
        )
        term = lax.dot_general(
            whigh[:, lanes], map_lo[b], dims, preferred_element_type=jnp.float32
        )
        term = both[:n] + (both[n:] + term)
        latent = term if latent is None else latent + term
    lat_out[...] = latent


def fit(place, slots, inverse0, weight0, hi, lo, pixel_total):
    n, freqs = weight0.shape
    parts = hi.shape[0] // 2
    return call(
        functools.partial(fit_kernel, pixel_total, parts),
        [(n, freqs // parts), (1, 1), (n, hi.shape[1])],
        place, *slots, inverse0, weight0, hi, lo,
        name="fit",
        scratch=[VM((freqs, freqs), jnp.bfloat16)] * 3 + [VM((n, freqs), jnp.float32)],
    )


def clean_kernel(parts, place, *refs):
    latents, loads, first, second, out = refs[:parts], *refs[parts:]
    width = first.shape[2]
    rows = latents[0].shape[1]
    for k in range(parts):
        at = lax.rem(place[1] + parts - k, parts)
        model = thin(latents[k][...], loads[...], ((0,), (0,)))
        here = pl.ds(pl.multiple_of(at * rows, rows), rows)
        out[here, 0:width] = first[at, 0:rows] - model[:, 0:width]
        out[here, width:] = second[at, 0:rows] - model[:, width:]


def clean(place, first, second, latents, loads):
    parts, _, width = first.shape
    rows = latents[0].shape[1]
    kernel = functools.partial(clean_kernel, parts)
    shape = (parts * rows, 2 * width)
    return call(kernel, [shape], place, *latents, loads, first, second, name="clean")[0]


def body(sky_maps, validity, row_taps, column_taps, init_loadings):
    rows_here, cols_here, freqs_here = sky_maps.shape
    sx, sy, af = (lax.axis_size(a) for a in ("sx", "sy", "af"))
    width = freqs_here // 2
    n = init_loadings.shape[1]
    pixels_here = rows_here * cols_here
    pixels = pixels_here // af
    place = jnp.stack([lax.rem(lax.axis_index("sx"), 2), lax.axis_index("af")]).astype(jnp.int32)
    mask = validity.astype(jnp.float32)[:, :, None]

    def halos(block, axis, count):
        low = lax.ppermute(block, axis, [(i, i + 1) for i in range(count - 1)])
        high = lax.ppermute(block, axis, [(i + 1, i) for i in range(count - 1)])
        return low, high

    def shifted(block, k):
        return lax.ppermute(block, "af", [(i, (i + k) % af) for i in range(af)])

    def swapped(block):
        return lax.ppermute(block, "sx", [(i, i ^ 1) for i in range(sx)])

    beamed, traded = [], []
    masked = [sky_maps[:, :, h * width : (h + 1) * width] * mask for h in range(2)]
    around = [halos(m, "sx", sx) for m in masked]
    for h in range(2):
        smoothed = beam(around[h][0], masked[h], around[h][1], row_taps.T, h)
        smoothed = smoothed.reshape(cols_here, rows_here, width)
        low, high = halos(smoothed, "sy", sy)
        spectra = beam(low, smoothed, high, column_taps.T, h, init_loadings.T)
        spectra = spectra.reshape(af, pixels + n, width)
        beamed.append(spectra)
        traded.append(lax.all_to_all(spectra, "af", 0, 0))
    even, odd = traded

    theirs, partial, hi, lo = moments(place, even, odd, pixels)
    partial = partial + swapped(theirs)
    inverse0, weight0 = first_weights(even, odd, n)
    piece = partial[0]
    for k in range(1, af):
        piece = piece + shifted(partial[k], k)
    piece, inverse0, weight0 = lax.optimization_barrier((piece, inverse0, weight0))
    ranks = sx * sy // 2
    groups = [[s * sy + t for s in range(c, sx, 2) for t in range(sy)] for c in range(2)]
    shape = piece.shape
    pieces = piece.reshape(ranks, -1, shape[1])
    pieces = lax.all_to_all(pieces, ("sx", "sy"), 0, 0, axis_index_groups=groups)
    owned = jnp.sum(pieces, axis=0)
    pieces = lax.all_to_all(
        jnp.broadcast_to(owned[None], pieces.shape), ("sx", "sy"), 0, 0, axis_index_groups=groups
    )
    piece = pieces.reshape(shape)
    mine = [piece] + [shifted(piece, k) for k in range(1, af)]
    other = [swapped(x) for x in mine]

    loads_here, noise, latent = fit(
        place, mine + other, inverse0, weight0, hi, lo, float(pixels_here * sx * sy)
    )
    latents = [latent] + [shifted(latent, k) for k in range(1, af)]
    cleaned = clean(place, beamed[0], beamed[1], latents, loads_here)
    return cleaned.reshape(rows_here, cols_here, freqs_here), loads_here.T, noise.reshape(())


def solution(mesh):
    placed = (P("sx", "sy", "af"), P("sx", "sy"), P("af", None), P("af", None), P("af", None))
    return jax.shard_map(
        body,
        mesh=mesh,
        in_specs=placed,
        out_specs=(P("sx", "sy", "af"), P("af", None), P()),
        check_vma=False,
    )
```

```python
import functools

import jax
import jax.numpy as jnp
from jax import lax
from jax.experimental import pallas as pl
from jax.experimental.pallas import tpu as pltpu
from jax.sharding import PartitionSpec as P

ITERS = 4
HI = lax.Precision.HIGHEST
VM = pltpu.VMEM
INTERPRET = False
LIMIT = 32 << 20


def call(kernel, out_shapes, *args, name, scratch=(), dtypes=None):
    dtypes = dtypes or [jnp.float32] * len(out_shapes)
    fast = pl.BlockSpec(memory_space=VM)
    specs = [
        pl.BlockSpec(memory_space=pltpu.SMEM) if x.dtype == jnp.int32 else fast for x in args
    ]
    if INTERPRET:
        outs = [jax.ShapeDtypeStruct(s, d) for s, d in zip(out_shapes, dtypes)]
    else:
        outs = [VM(s, d) for s, d in zip(out_shapes, dtypes)]
        args = [
            x if x.dtype == jnp.int32 else pltpu.with_memory_space_constraint(x, VM) for x in args
        ]
    return pl.pallas_call(
        kernel,
        out_shape=outs,
        in_specs=specs,
        out_specs=[fast] * len(outs),
        scratch_shapes=list(scratch),
        compiler_params=pltpu.CompilerParams(vmem_limit_bytes=LIMIT),
        interpret=INTERPRET,
        name=name,
    )(*args)


def contract(left, right, dims):
    return lax.dot_general(
        left, right, (dims, ((), ())), precision=HI, preferred_element_type=jnp.float32
    )


def split3(x):
    hi = x.astype(jnp.bfloat16)
    rest = x - hi.astype(jnp.float32)
    mid = rest.astype(jnp.bfloat16)
    low = (rest - mid.astype(jnp.float32)).astype(jnp.bfloat16)
    return hi, mid, low


def thin(left, right, dims):
    (ld,), (rd,) = dims
    lh, lm, ll = split3(left)
    rh, rm, rl = split3(right)
    a = jnp.concatenate([ll, lm, lh, lm, lh, lh], axis=ld)
    b = jnp.concatenate([rh, rm, rl, rh, rm, rh], axis=rd)
    return lax.dot_general(a, b, (dims, ((), ())), preferred_element_type=jnp.float32)


def beam_kernel(half, low, own, high, taps, *rest):
    out = rest[-1]
    length, wide, width = own.shape
    count = taps.shape[0]
    refs = (low, own, high)
    lanes = slice(half * width, (half + 1) * width)

    def strip(j, _):
        at = pl.ds(pl.multiple_of(j * 8, 8), 8)
        for block in range(length // 8):
            acc = [None] * 8
            held = {}
            for k in range(count + 7):
                row = block * 8 + k
                value = refs[row // length][row % length, at, :]
                if k < count:
                    held[k] = jnp.broadcast_to(taps[k : k + 1, lanes], value.shape)
                for i in range(8):
                    t = k - i
                    if 0 <= t < count:
                        term = held[t] * value
                        acc[i] = term if acc[i] is None else acc[i] + term
            out[j, 0:8, block * 8 : block * 8 + 8, :] = jnp.swapaxes(jnp.stack(acc), 0, 1)
        if len(rest) == 2:
            for e in range(out.shape[1] - 8):
                out[j, 8 + e] = rest[0][e * length : (e + 1) * length, lanes]

    lax.fori_loop(0, wide // 8, strip, None)


def beam(low, own, high, taps, half, loads=None):
    a, b, f = own.shape
    assert taps.shape[0] == 2 * a + 1
    more = [] if loads is None else [loads]
    extra = 0 if loads is None else loads.shape[0] // a
    shape = (b // 8, 8 + extra, a, f)
    kernel = functools.partial(beam_kernel, half)
    return call(kernel, [shape], low, own, high, taps, *more, name="beam")[0]


def row_block(place, c, k, parts):
    return lax.rem(place[0] + c, 2) * parts + lax.rem(place[1] + k, parts)


def moment_kernel(c, pixels, place, *refs):
    if len(refs) == 5:
        even, odd, out, hi, lo = refs
        parts = even.shape[0]
        for b in range(2 * parts):
            value = (even, odd)[b % 2][b // 2, 0:pixels]
            top = value.astype(jnp.bfloat16)
            hi[b] = top
            lo[b] = (value - top.astype(jnp.float32)).astype(jnp.bfloat16)
    else:
        hi, lo, out = refs
        parts = hi.shape[0] // 2
    blocks = 2 * parts
    width = hi.shape[2]
    half = width // 2
    dims = (((0,), (0,)), ((), ()))
    upper = lax.rem(place[0] + c, 2) == 0
    for k in range(parts):
        i = row_block(place, c, k, parts)
        at = [lax.rem(i + j, blocks) for j in range(parts)]
        left = jnp.concatenate([lo[i], hi[i], hi[i]], axis=0)
        high = jnp.concatenate([hi[b] for b in at], axis=1)
        low = jnp.concatenate([lo[b] for b in at], axis=1)
        right = jnp.concatenate([high, low, high], axis=0)
        block = lax.dot_general(left, right, dims, preferred_element_type=jnp.float32)
        for j in range(parts):
            out[k, j * width : (j + 1) * width, :] = block[:, j * width : (j + 1) * width]
        m = lax.rem(i, parts)
        left = jnp.concatenate([lo[m], hi[m], hi[m]], axis=0)
        left = jnp.where(upper, left[:, :half], left[:, half:])
        m = m + parts
        right = jnp.concatenate([hi[m], lo[m], hi[m]], axis=0)
        out[k, parts * width :, :] = lax.dot_general(
            left, right, dims, preferred_element_type=jnp.float32
        )


def moments(place, even, odd, pixels):
    parts, _, width = even.shape
    shape = (parts, width * parts + width // 2, width)
    halves = (2 * parts, pixels, width)
    half = jnp.bfloat16
    theirs, hi, lo = call(
        functools.partial(moment_kernel, 1, pixels), [shape, halves, halves], place, even, odd,
        name="moments", dtypes=[jnp.float32, half, half],
    )
    ours = call(functools.partial(moment_kernel, 0, pixels), [shape], place, hi, lo, name="moments")
    return theirs, ours[0], hi, lo


def every(tile, r):
    return jnp.broadcast_to(tile[r : r + 1], tile.shape)


def along(tile, k):
    return jnp.broadcast_to(tile[:, k : k + 1], tile.shape)


def inverse_spd(matrix):
    n = matrix.shape[0]
    lane = lax.broadcasted_iota(jnp.int32, (8, n), 1)
    row = lax.broadcasted_iota(jnp.int32, (8, n), 0)
    tiles = [matrix[i : i + 8] for i in range(0, n, 8)]
    for p in range(n // 8):
        cols = [[along(t, 8 * p + j) for t in tiles] for j in range(8)]
        for r in range(8):
            k = 8 * p + r
            top = every(tiles[p], r)
            heads = [
                along(top, 8 * p + j) if r == 0 else every(cols[j][p], r) for j in range(r, 8)
            ]
            pivot = 1.0 / heads[0]
            first = jnp.where(lane == k, 1.0, top) * pivot
            left = cols[r]
            for j in range(r + 1, 8):
                factor = heads[j - r] * pivot
                cols[j] = [t - x * factor for t, x in zip(cols[j], left)]
                cols[j][p] = jnp.where(row == r, factor, cols[j][p])
            tiles = [jnp.where(lane == k, 0.0, t) - x * first for t, x in zip(tiles, left)]
            tiles[p] = jnp.where(row == r, first, tiles[p])
    return jnp.concatenate(tiles, axis=0)


def total(x):
    return jnp.sum(jnp.sum(x, axis=1, keepdims=True), axis=0, keepdims=True)


def identity(n):
    return lax.broadcasted_iota(jnp.int32, (n, n), 0) == lax.broadcasted_iota(jnp.int32, (n, n), 1)


def parts_of(x):
    return jnp.concatenate(split3(x), axis=0)


def gram_of(left, right):
    n = left.shape[0] // 3
    grid = lax.dot_general(
        left, right, (((1,), (1,)), ((), ())), preferred_element_type=jnp.float32
    )
    rows = grid[:n] + (grid[n : 2 * n] + grid[2 * n :])
    return rows[:, :n] + (rows[:, n : 2 * n] + rows[:, 2 * n :])


def times(matrix, right):
    n = matrix.shape[0]
    top, mid, low = split3(matrix)
    left = jnp.concatenate([low, mid, top, mid, top, top], axis=1)
    right = jnp.concatenate([right, right[: 2 * n], right[:n]], axis=0)
    return jnp.dot(left, right, preferred_element_type=jnp.float32)


def weights(pieces, gram, noise):
    inverse = inverse_spd(gram + jnp.where(identity(gram.shape[0]), noise, 0.0))
    return inverse, times(inverse, pieces)


def first_kernel(even, odd, inverse_out, weight_out):
    n = weight_out.shape[0]
    rows = even.shape[1]
    loads = jnp.concatenate(
        [ref[b, rows - n : rows] for b in range(even.shape[0]) for ref in (even, odd)], axis=1
    )
    pieces = parts_of(loads)
    gram = gram_of(pieces, pieces)
    inverse_out[...], weight_out[...] = weights(pieces, gram, jnp.ones((1, 1), jnp.float32))


def first_weights(even, odd, n):
    parts, _, width = even.shape
    return call(first_kernel, [(n, n), (n, 2 * parts * width)], even, odd, name="first")


def cross_of(stacked, hi, mid, low):
    n = stacked.shape[0] // 3

    def product(count, ref):
        return jnp.dot(stacked[: count * n], ref[...], preferred_element_type=jnp.float32)

    top, middle, last = product(3, hi), product(2, mid), product(1, low)
    small = top[2 * n :] + middle[n:] + last
    return top[:n] + (top[n : 2 * n] + middle[:n] + small)


def fit_kernel(pixel_total, parts, place, *refs):
    slots = refs[: 2 * parts]
    inverse0, weight0, map_hi, map_lo = refs[2 * parts : 2 * parts + 4]
    block_out, noise_out, lat_out, hi, mid, low, held = refs[2 * parts + 4 :]
    width = slots[0].shape[1]
    blocks = 2 * parts
    freqs = blocks * width
    n = weight0.shape[0]
    diagonal = identity(width)
    power = jnp.zeros((width, width), jnp.float32)

    def place_block(i, j, block, mirror):
        rows = pl.ds(pl.multiple_of(i * width, width), width)
        cols = pl.ds(pl.multiple_of(j * width, width), width)
        for dest, value in zip((hi, mid, low), split3(block)):
            dest[rows, cols] = value
        if mirror:
            for dest, value in zip((hi, mid, low), split3(block.T)):
                dest[cols, rows] = value

    for s, ref in enumerate(slots):
        i = row_block(place, s // parts, parts - s % parts, parts)
        for j in range(parts):
            place_block(i, lax.rem(i + j, blocks), ref[j * width : (j + 1) * width], j > 0)
        power = power + jnp.where(diagonal, ref[:width], 0.0)
    upper = place[0] == 0
    for k in range(parts):
        m = lax.rem(place[1] + parts - k, parts)
        ours, theirs = slots[k][parts * width :], slots[parts + k][parts * width :]
        block = jnp.concatenate(
            [jnp.where(upper, ours, theirs), jnp.where(upper, theirs, ours)], axis=0
        )
        place_block(m, m + parts, block, True)
    power = total(power)

    def step(_, state):
        inverse, weight, noise = state
        stacked = parts_of(weight)
        cross = cross_of(stacked, hi, mid, low)
        pieces = parts_of(cross)
        scaled = pixel_total * noise * inverse + gram_of(pieces, stacked)
        updated = times(inverse_spd(scaled), pieces)
        held[...] = updated
        pieces = parts_of(updated)
        gram = gram_of(pieces, pieces)
        noise = (power - 2.0 * total(updated * cross) + total(scaled * gram)) / (
            pixel_total * freqs
        )
        return (*weights(pieces, gram, noise), noise)

    state = (inverse0[...], weight0[...], jnp.ones((1, 1), jnp.float32))
    _, weight, noise = lax.fori_loop(0, ITERS, step, state)
    noise_out[...] = noise
    here = block_out.shape[1]
    block_out[...] = held[:, pl.ds(pl.multiple_of(place[1] * here, here), here)]
    whigh, wlow, _ = split3(weight)
    pair = jnp.concatenate([whigh, wlow], axis=0)
    latent = None
    for b in range(blocks):
        lanes = slice(b * width, (b + 1) * width)
        dims = (((1,), (1,)), ((), ()))
        both = lax.dot_general(
            pair[:, lanes], map_hi[b], dims, preferred_element_type=jnp.float32
        )
        term = lax.dot_general(
            whigh[:, lanes], map_lo[b], dims, preferred_element_type=jnp.float32
        )
        term = both[:n] + (both[n:] + term)
        latent = term if latent is None else latent + term
    lat_out[...] = latent


def fit(place, slots, inverse0, weight0, hi, lo, pixel_total):
    n, freqs = weight0.shape
    parts = hi.shape[0] // 2
    return call(
        functools.partial(fit_kernel, pixel_total, parts),
        [(n, freqs // parts), (1, 1), (n, hi.shape[1])],
        place, *slots, inverse0, weight0, hi, lo,
        name="fit",
        scratch=[VM((freqs, freqs), jnp.bfloat16)] * 3 + [VM((n, freqs), jnp.float32)],
    )


def clean_kernel(parts, place, *refs):
    latents, loads, first, second, out = refs[:parts], *refs[parts:]
    width = first.shape[2]
    rows = latents[0].shape[1]
    for k in range(parts):
        at = lax.rem(place[1] + parts - k, parts)
        model = thin(latents[k][...], loads[...], ((0,), (0,)))
        here = pl.ds(pl.multiple_of(at * rows, rows), rows)
        out[here, 0:width] = first[at, 0:rows] - model[:, 0:width]
        out[here, width:] = second[at, 0:rows] - model[:, width:]


def clean(place, first, second, latents, loads):
    parts, _, width = first.shape
    rows = latents[0].shape[1]
    kernel = functools.partial(clean_kernel, parts)
    shape = (parts * rows, 2 * width)
    return call(kernel, [shape], place, *latents, loads, first, second, name="clean")[0]


def body(sky_maps, validity, row_taps, column_taps, init_loadings):
    rows_here, cols_here, freqs_here = sky_maps.shape
    sx, sy, af = (lax.axis_size(a) for a in ("sx", "sy", "af"))
    width = freqs_here // 2
    n = init_loadings.shape[1]
    pixels_here = rows_here * cols_here
    pixels = pixels_here // af
    place = jnp.stack([lax.rem(lax.axis_index("sx"), 2), lax.axis_index("af")]).astype(jnp.int32)
    mask = validity.astype(jnp.float32)[:, :, None]

    def halos(block, axis, count):
        low = lax.ppermute(block, axis, [(i, i + 1) for i in range(count - 1)])
        high = lax.ppermute(block, axis, [(i + 1, i) for i in range(count - 1)])
        return low, high

    def shifted(block, k):
        return lax.ppermute(block, "af", [(i, (i + k) % af) for i in range(af)])

    def swapped(block):
        return lax.ppermute(block, "sx", [(i, i ^ 1) for i in range(sx)])

    beamed, traded = [], []
    masked = [sky_maps[:, :, h * width : (h + 1) * width] * mask for h in range(2)]
    around = [halos(m, "sx", sx) for m in masked]
    for h in range(2):
        smoothed = beam(around[h][0], masked[h], around[h][1], row_taps.T, h)
        smoothed = smoothed.reshape(cols_here, rows_here, width)
        low, high = halos(smoothed, "sy", sy)
        spectra = beam(low, smoothed, high, column_taps.T, h, init_loadings.T)
        spectra = spectra.reshape(af, pixels + n, width)
        beamed.append(spectra)
        traded.append(lax.all_to_all(spectra, "af", 0, 0))
    even, odd = traded

    theirs, partial, hi, lo = moments(place, even, odd, pixels)
    partial = partial + swapped(theirs)
    inverse0, weight0 = first_weights(even, odd, n)
    piece = partial[0]
    for k in range(1, af):
        piece = piece + shifted(partial[k], k)
    piece, inverse0, weight0 = lax.optimization_barrier((piece, inverse0, weight0))
    ranks = sx * sy // 2
    groups = [[s * sy + t for s in range(c, sx, 2) for t in range(sy)] for c in range(2)]
    shape = piece.shape
    pieces = piece.reshape(-1, 2, shape[1])
    pieces = lax.all_to_all(
        pieces, ("sx", "sy"), 0, 0, axis_index_groups=groups, tiled=True
    )
    owned = jnp.sum(pieces.reshape(ranks, -1, 2, shape[1]), axis=0)
    pieces = jnp.broadcast_to(owned[None], (ranks, *owned.shape)).reshape(pieces.shape)
    pieces = lax.all_to_all(
        pieces, ("sx", "sy"), 0, 0, axis_index_groups=groups, tiled=True
    )
    piece = pieces.reshape(shape)
    mine = [piece] + [shifted(piece, k) for k in range(1, af)]
    other = [swapped(x) for x in mine]

    loads_here, noise, latent = fit(
        place, mine + other, inverse0, weight0, hi, lo, float(pixels_here * sx * sy)
    )
    latents = [latent] + [shifted(latent, k) for k in range(1, af)]
    cleaned = clean(place, beamed[0], beamed[1], latents, loads_here)
    return cleaned.reshape(rows_here, cols_here, freqs_here), loads_here.T, noise.reshape(())


def solution(mesh):
    placed = (P("sx", "sy", "af"), P("sx", "sy"), P("af", None), P("af", None), P("af", None))
    return jax.shard_map(
        body,
        mesh=mesh,
        in_specs=placed,
        out_specs=(P("sx", "sy", "af"), P("af", None), P()),
        check_vma=False,
    )
```

```python
import functools

import jax
import jax.numpy as jnp
from jax import lax
from jax.experimental import pallas as pl
from jax.experimental.pallas import tpu as pltpu
from jax.sharding import PartitionSpec as P

ITERS = 4
HI = lax.Precision.HIGHEST
VM = pltpu.VMEM
INTERPRET = False
LIMIT = 32 << 20


def call(kernel, out_shapes, *args, name, scratch=(), dtypes=None, out_space=VM):
    dtypes = dtypes or [jnp.float32] * len(out_shapes)
    fast = pl.BlockSpec(memory_space=VM)
    specs = [
        pl.BlockSpec(memory_space=pltpu.SMEM) if x.dtype == jnp.int32 else fast for x in args
    ]
    if INTERPRET or out_space is not VM:
        outs = [jax.ShapeDtypeStruct(s, d) for s, d in zip(out_shapes, dtypes)]
    else:
        outs = [VM(s, d) for s, d in zip(out_shapes, dtypes)]
    if not INTERPRET:
        args = [
            x if x.dtype == jnp.int32 else pltpu.with_memory_space_constraint(x, VM) for x in args
        ]
    return pl.pallas_call(
        kernel,
        out_shape=outs,
        in_specs=specs,
        out_specs=[pl.BlockSpec(memory_space=out_space)] * len(outs),
        scratch_shapes=list(scratch),
        compiler_params=pltpu.CompilerParams(vmem_limit_bytes=LIMIT),
        interpret=INTERPRET,
        name=name,
    )(*args)


def contract(left, right, dims):
    return lax.dot_general(
        left, right, (dims, ((), ())), precision=HI, preferred_element_type=jnp.float32
    )


def split3(x):
    hi = x.astype(jnp.bfloat16)
    rest = x - hi.astype(jnp.float32)
    mid = rest.astype(jnp.bfloat16)
    low = (rest - mid.astype(jnp.float32)).astype(jnp.bfloat16)
    return hi, mid, low


def thin(left, right, dims):
    (ld,), (rd,) = dims
    lh, lm, ll = split3(left)
    rh, rm, rl = split3(right)
    a = jnp.concatenate([ll, lm, lh, lm, lh, lh], axis=ld)
    b = jnp.concatenate([rh, rm, rl, rh, rm, rh], axis=rd)
    return lax.dot_general(a, b, (dims, ((), ())), preferred_element_type=jnp.float32)


def strip(refs, taps, lanes, j, out):
    length = refs[1].shape[0]
    count = taps.shape[0]
    at = pl.ds(pl.multiple_of(j * 8, 8), 8)
    for block in range(length // 8):
        acc = [None] * 8
        held = {}
        for k in range(count + 7):
            row = block * 8 + k
            value = refs[row // length][row % length, at, :]
            if k < count:
                held[k] = jnp.broadcast_to(taps[k : k + 1, lanes], value.shape)
            for i in range(8):
                t = k - i
                if 0 <= t < count:
                    term = held[t] * value
                    acc[i] = term if acc[i] is None else acc[i] + term
        out[0:8, block * 8 : block * 8 + 8, :] = jnp.swapaxes(jnp.stack(acc), 0, 1)


def lanes_of(half, own):
    return slice(half * own.shape[2], (half + 1) * own.shape[2])


def beam_kernel(half, low, own, high, taps, out):
    def one(j, _):
        strip((low, own, high), taps, lanes_of(half, own), j, out.at[j])

    lax.fori_loop(0, own.shape[1] // 8, one, None)


def beam(low, own, high, taps, half):
    a, b, f = own.shape
    assert taps.shape[0] == 2 * a + 1
    kernel = functools.partial(beam_kernel, half)
    return call(kernel, [(b // 8, 8, a, f)], low, own, high, taps, name="beam")[0]


def parted_kernel(half, place, low, own, high, taps, loads, *outs):
    parts = len(outs)
    length = own.shape[0]
    lanes = lanes_of(half, own)
    for k, out in enumerate(outs):
        strip((low, own, high), taps, lanes, lax.rem(place[1] + k, parts), out)
        for e in range(out.shape[0] - 8):
            out[8 + e] = loads[e * length : (e + 1) * length, lanes]


def parted_beam(place, low, own, high, taps, half, loads, parts):
    a, b, f = own.shape
    assert taps.shape[0] == 2 * a + 1 and b == 8 * parts
    shape = (8 + loads.shape[0] // a, a, f)
    kernel = functools.partial(parted_kernel, half)
    outs = call(kernel, [shape] * parts, place, low, own, high, taps, loads, name="beam")
    return [x.reshape(-1, f) for x in outs]


def source(place, k, parts):
    return lax.rem(place[1] + parts - k, parts)


def row_block(place, c, k, parts):
    return lax.rem(place[0] + c, 2) * parts + lax.rem(place[1] + k, parts)


def moment_kernel(c, pixels, place, *refs):
    if len(refs) > 3:
        out, hi, lo = refs[-3:]
        parts = hi.shape[0] // 2
        for s in range(2 * parts):
            value = refs[s][0:pixels]
            top = value.astype(jnp.bfloat16)
            b = 2 * source(place, s % parts, parts) + s // parts
            hi[b] = top
            lo[b] = (value - top.astype(jnp.float32)).astype(jnp.bfloat16)
    else:
        hi, lo, out = refs
        parts = hi.shape[0] // 2
    blocks = 2 * parts
    width = hi.shape[2]
    half = width // 2
    dims = (((0,), (0,)), ((), ()))
    upper = lax.rem(place[0] + c, 2) == 0
    for k in range(parts):
        i = row_block(place, c, k, parts)
        at = [lax.rem(i + j, blocks) for j in range(parts)]
        left = jnp.concatenate([lo[i], hi[i], hi[i]], axis=0)
        high = jnp.concatenate([hi[b] for b in at], axis=1)
        low = jnp.concatenate([lo[b] for b in at], axis=1)
        right = jnp.concatenate([high, low, high], axis=0)
        block = lax.dot_general(left, right, dims, preferred_element_type=jnp.float32)
        for j in range(parts):
            out[k, j * width : (j + 1) * width, :] = block[:, j * width : (j + 1) * width]
        m = lax.rem(i, parts)
        left = jnp.concatenate([lo[m], hi[m], hi[m]], axis=0)
        left = jnp.where(upper, left[:, :half], left[:, half:])
        m = m + parts
        right = jnp.concatenate([hi[m], lo[m], hi[m]], axis=0)
        out[k, parts * width :, :] = lax.dot_general(
            left, right, dims, preferred_element_type=jnp.float32
        )


def moments(place, slots, pixels):
    width = slots[0].shape[1]
    parts = len(slots) // 2
    shape = (parts, width * parts + width // 2, width)
    halves = (2 * parts, pixels, width)
    half = jnp.bfloat16
    theirs, hi, lo = call(
        functools.partial(moment_kernel, 1, pixels), [shape, halves, halves], place, *slots,
        name="moments", dtypes=[jnp.float32, half, half],
    )
    ours = call(functools.partial(moment_kernel, 0, pixels), [shape], place, hi, lo, name="moments")
    return theirs, ours[0], hi, lo


def every(tile, r):
    return jnp.broadcast_to(tile[r : r + 1], tile.shape)


def along(tile, k):
    return jnp.broadcast_to(tile[:, k : k + 1], tile.shape)


def inverse_spd(matrix):
    n = matrix.shape[0]
    lane = lax.broadcasted_iota(jnp.int32, (8, n), 1)
    row = lax.broadcasted_iota(jnp.int32, (8, n), 0)
    tiles = [matrix[i : i + 8] for i in range(0, n, 8)]
    for p in range(n // 8):
        cols = [[along(t, 8 * p + j) for t in tiles] for j in range(8)]
        for r in range(8):
            k = 8 * p + r
            top = every(tiles[p], r)
            heads = [
                along(top, 8 * p + j) if r == 0 else every(cols[j][p], r) for j in range(r, 8)
            ]
            pivot = 1.0 / heads[0]
            first = jnp.where(lane == k, 1.0, top) * pivot
            left = cols[r]
            for j in range(r + 1, 8):
                factor = heads[j - r] * pivot
                cols[j] = [t - x * factor for t, x in zip(cols[j], left)]
                cols[j][p] = jnp.where(row == r, factor, cols[j][p])
            tiles = [jnp.where(lane == k, 0.0, t) - x * first for t, x in zip(tiles, left)]
            tiles[p] = jnp.where(row == r, first, tiles[p])
    return jnp.concatenate(tiles, axis=0)


def total(x):
    return jnp.sum(jnp.sum(x, axis=1, keepdims=True), axis=0, keepdims=True)


def identity(n):
    return lax.broadcasted_iota(jnp.int32, (n, n), 0) == lax.broadcasted_iota(jnp.int32, (n, n), 1)


def parts_of(x):
    return jnp.concatenate(split3(x), axis=0)


def gram_of(left, right):
    n = left.shape[0] // 3
    grid = lax.dot_general(
        left, right, (((1,), (1,)), ((), ())), preferred_element_type=jnp.float32
    )
    rows = grid[:n] + (grid[n : 2 * n] + grid[2 * n :])
    return rows[:, :n] + (rows[:, n : 2 * n] + rows[:, 2 * n :])


def times(matrix, right):
    n = matrix.shape[0]
    top, mid, low = split3(matrix)
    left = jnp.concatenate([low, mid, top, mid, top, top], axis=1)
    right = jnp.concatenate([right, right[: 2 * n], right[:n]], axis=0)
    return jnp.dot(left, right, preferred_element_type=jnp.float32)


def weights(pieces, gram, noise):
    inverse = inverse_spd(gram + jnp.where(identity(gram.shape[0]), noise, 0.0))
    return inverse, times(inverse, pieces)


def first_kernel(place, *refs):
    slots, (inverse_out, weight_out, loads) = refs[:-3], refs[-3:]
    parts = len(slots) // 2
    n = weight_out.shape[0]
    rows, width = slots[0].shape
    for s, ref in enumerate(slots):
        b = 2 * source(place, s % parts, parts) + s // parts
        loads[:, pl.ds(pl.multiple_of(b * width, width), width)] = ref[rows - n : rows]
    pieces = parts_of(loads[...])
    gram = gram_of(pieces, pieces)
    inverse_out[...], weight_out[...] = weights(pieces, gram, jnp.ones((1, 1), jnp.float32))


def first_weights(place, slots, n):
    shape = (n, len(slots) * slots[0].shape[1])
    scratch = [VM(shape, jnp.float32)]
    return call(first_kernel, [(n, n), shape], place, *slots, name="first", scratch=scratch)


def cross_of(stacked, hi, lo):
    n = stacked.shape[0] // 3
    top = jnp.dot(stacked, hi[...], preferred_element_type=jnp.float32)
    low = jnp.dot(stacked[: 2 * n], lo[...], preferred_element_type=jnp.float32)
    return top[:n] + (top[n : 2 * n] + low[:n] + (top[2 * n :] + low[n:]))


def fit_kernel(pixel_total, parts, place, *refs):
    slots = refs[: 2 * parts]
    inverse0, weight0, map_hi, map_lo = refs[2 * parts : 2 * parts + 4]
    block_out, noise_out, lat_out, hi, lo, held = refs[2 * parts + 4 :]
    width = slots[0].shape[1]
    blocks = 2 * parts
    freqs = blocks * width
    n = weight0.shape[0]
    diagonal = identity(width)
    power = jnp.zeros((width, width), jnp.float32)

    def place_block(i, j, block, mirror):
        rows = pl.ds(pl.multiple_of(i * width, width), width)
        cols = pl.ds(pl.multiple_of(j * width, width), width)
        top, rest, _ = split3(block)
        hi[rows, cols], lo[rows, cols] = top, rest
        if mirror:
            top, rest, _ = split3(block.T)
            hi[cols, rows], lo[cols, rows] = top, rest

    for s, ref in enumerate(slots):
        i = row_block(place, s // parts, parts - s % parts, parts)
        for j in range(parts):
            place_block(i, lax.rem(i + j, blocks), ref[j * width : (j + 1) * width], j > 0)
        power = power + jnp.where(diagonal, ref[:width], 0.0)
    upper = place[0] == 0
    for k in range(parts):
        m = lax.rem(place[1] + parts - k, parts)
        ours, theirs = slots[k][parts * width :], slots[parts + k][parts * width :]
        block = jnp.concatenate(
            [jnp.where(upper, ours, theirs), jnp.where(upper, theirs, ours)], axis=0
        )
        place_block(m, m + parts, block, True)
    power = total(power)

    def step(_, state):
        inverse, weight, noise = state
        stacked = parts_of(weight)
        cross = cross_of(stacked, hi, lo)
        pieces = parts_of(cross)
        scaled = pixel_total * noise * inverse + gram_of(pieces, stacked)
        updated = times(inverse_spd(scaled), pieces)
        held[...] = updated
        pieces = parts_of(updated)
        gram = gram_of(pieces, pieces)
        noise = (power - 2.0 * total(updated * cross) + total(scaled * gram)) / (
            pixel_total * freqs
        )
        return (*weights(pieces, gram, noise), noise)

    state = (inverse0[...], weight0[...], jnp.ones((1, 1), jnp.float32))
    _, weight, noise = lax.fori_loop(0, ITERS, step, state)
    noise_out[...] = noise
    here = block_out.shape[1]
    block_out[...] = held[:, pl.ds(pl.multiple_of(place[1] * here, here), here)]
    whigh, wlow, _ = split3(weight)
    pair = jnp.concatenate([whigh, wlow], axis=0)
    latent = None
    for b in range(blocks):
        lanes = slice(b * width, (b + 1) * width)
        dims = (((1,), (1,)), ((), ()))
        both = lax.dot_general(
            pair[:, lanes], map_hi[b], dims, preferred_element_type=jnp.float32
        )
        term = lax.dot_general(
            whigh[:, lanes], map_lo[b], dims, preferred_element_type=jnp.float32
        )
        term = both[:n] + (both[n:] + term)
        latent = term if latent is None else latent + term
    lat_out[...] = latent


def fit(place, slots, inverse0, weight0, hi, lo, pixel_total):
    n, freqs = weight0.shape
    parts = hi.shape[0] // 2
    return call(
        functools.partial(fit_kernel, pixel_total, parts),
        [(n, freqs // parts), (1, 1), (n, hi.shape[1])],
        place, *slots, inverse0, weight0, hi, lo,
        name="fit",
        scratch=[VM((freqs, freqs), jnp.bfloat16)] * 2 + [VM((n, freqs), jnp.float32)],
    )


def clean_kernel(parts, place, *refs):
    latents, loads, slots = refs[:parts], refs[parts], refs[parts + 1 : 3 * parts + 1]
    out, held, sems = refs[3 * parts + 1 :]
    width = slots[0].shape[1]
    rows = latents[0].shape[1]
    copies = []
    for k in range(parts):
        model = thin(latents[k][...], loads[...], ((0,), (0,)))
        for h in range(2):
            lanes = slice(h * width, (h + 1) * width)
            held[k, :, lanes] = slots[h * parts + (parts - k) % parts][0:rows] - model[:, lanes]
        here = pl.ds(pl.multiple_of(source(place, k, parts) * rows, rows), rows)
        copies.append(pltpu.make_async_copy(held.at[k], out.at[here], sems.at[k]))
        copies[-1].start()
    for copy in copies:
        copy.wait()


def clean(place, slots, latents, loads):
    parts = len(latents)
    rows = latents[0].shape[1]
    wide = 2 * slots[0].shape[1]
    return call(
        functools.partial(clean_kernel, parts), [(parts * rows, wide)],
        place, *latents, loads, *slots,
        name="clean",
        scratch=[VM((parts, rows, wide), jnp.float32), pltpu.SemaphoreType.DMA((parts,))],
        out_space=pl.ANY,
    )[0]


def body(sky_maps, validity, row_taps, column_taps, init_loadings):
    rows_here, cols_here, freqs_here = sky_maps.shape
    sx, sy, af = (lax.axis_size(a) for a in ("sx", "sy", "af"))
    width = freqs_here // 2
    n = init_loadings.shape[1]
    pixels_here = rows_here * cols_here
    pixels = pixels_here // af
    place = jnp.stack([lax.rem(lax.axis_index("sx"), 2), lax.axis_index("af")]).astype(jnp.int32)
    mask = validity.astype(jnp.float32)[:, :, None]

    def halos(block, axis, count):
        low = lax.ppermute(block, axis, [(i, i + 1) for i in range(count - 1)])
        high = lax.ppermute(block, axis, [(i + 1, i) for i in range(count - 1)])
        return low, high

    def shifted(block, k):
        return lax.ppermute(block, "af", [(i, (i + k) % af) for i in range(af)])

    def swapped(block):
        return lax.ppermute(block, "sx", [(i, i ^ 1) for i in range(sx)])

    beamed, traded = [], []
    masked = [sky_maps[:, :, h * width : (h + 1) * width] * mask for h in range(2)]
    around = [halos(m, "sx", sx) for m in masked]
    for h in range(2):
        smoothed = beam(around[h][0], masked[h], around[h][1], row_taps.T, h)
        smoothed = smoothed.reshape(cols_here, rows_here, width)
        low, high = halos(smoothed, "sy", sy)
        slots = parted_beam(place, low, smoothed, high, column_taps.T, h, init_loadings.T, af)
        beamed += slots
        traded += slots[:1] + [shifted(slots[k], k) for k in range(1, af)]

    theirs, partial, hi, lo = moments(place, traded, pixels)
    partial = partial + swapped(theirs)
    inverse0, weight0 = first_weights(place, traded, n)
    piece = partial[0]
    for k in range(1, af):
        piece = piece + shifted(partial[k], k)
    piece, inverse0, weight0 = lax.optimization_barrier((piece, inverse0, weight0))
    ranks = sx * sy // 2
    groups = [[s * sy + t for s in range(c, sx, 2) for t in range(sy)] for c in range(2)]
    shape = piece.shape
    pieces = piece.reshape(-1, 2, shape[1])
    pieces = lax.all_to_all(
        pieces, ("sx", "sy"), 0, 0, axis_index_groups=groups, tiled=True
    )
    owned = jnp.sum(pieces.reshape(ranks, -1, 2, shape[1]), axis=0)
    pieces = jnp.broadcast_to(owned[None], (ranks, *owned.shape)).reshape(pieces.shape)
    pieces = lax.all_to_all(
        pieces, ("sx", "sy"), 0, 0, axis_index_groups=groups, tiled=True
    )
    piece = pieces.reshape(shape)
    mine = [piece] + [shifted(piece, k) for k in range(1, af)]
    other = [swapped(x) for x in mine]

    loads_here, noise, latent = fit(
        place, mine + other, inverse0, weight0, hi, lo, float(pixels_here * sx * sy)
    )
    latents = [latent] + [shifted(latent, k) for k in range(1, af)]
    cleaned = clean(place, beamed, latents, loads_here)
    return cleaned.reshape(rows_here, cols_here, freqs_here), loads_here.T, noise.reshape(())


def solution(mesh):
    placed = (P("sx", "sy", "af"), P("sx", "sy"), P("af", None), P("af", None), P("af", None))
    return jax.shard_map(
        body,
        mesh=mesh,
        in_specs=placed,
        out_specs=(P("sx", "sy", "af"), P("af", None), P()),
        check_vma=False,
    )
```

```python
import functools

import jax
import jax.numpy as jnp
from jax import lax
from jax.experimental import pallas as pl
from jax.experimental.pallas import tpu as pltpu
from jax.sharding import PartitionSpec as P

ITERS = 4
HI = lax.Precision.HIGHEST
VM = pltpu.VMEM
INTERPRET = False
LIMIT = 32 << 20


def call(kernel, out_shapes, *args, name, scratch=(), dtypes=None, out_space=VM):
    dtypes = dtypes or [jnp.float32] * len(out_shapes)
    fast = pl.BlockSpec(memory_space=VM)
    specs = [
        pl.BlockSpec(memory_space=pltpu.SMEM) if x.dtype == jnp.int32 else fast for x in args
    ]
    if INTERPRET or out_space is not VM:
        outs = [jax.ShapeDtypeStruct(s, d) for s, d in zip(out_shapes, dtypes)]
    else:
        outs = [VM(s, d) for s, d in zip(out_shapes, dtypes)]
    if not INTERPRET:
        args = [
            x if x.dtype == jnp.int32 else pltpu.with_memory_space_constraint(x, VM) for x in args
        ]
    return pl.pallas_call(
        kernel,
        out_shape=outs,
        in_specs=specs,
        out_specs=[pl.BlockSpec(memory_space=out_space)] * len(outs),
        scratch_shapes=list(scratch),
        compiler_params=pltpu.CompilerParams(vmem_limit_bytes=LIMIT),
        interpret=INTERPRET,
        name=name,
    )(*args)


def contract(left, right, dims):
    return lax.dot_general(
        left, right, (dims, ((), ())), precision=HI, preferred_element_type=jnp.float32
    )


def split3(x):
    hi = x.astype(jnp.bfloat16)
    rest = x - hi.astype(jnp.float32)
    mid = rest.astype(jnp.bfloat16)
    low = (rest - mid.astype(jnp.float32)).astype(jnp.bfloat16)
    return hi, mid, low


def thin(left, right, dims):
    (ld,), (rd,) = dims
    lh, lm, ll = split3(left)
    rh, rm, rl = split3(right)
    a = jnp.concatenate([ll, lm, lh, lm, lh, lh], axis=ld)
    b = jnp.concatenate([rh, rm, rl, rh, rm, rh], axis=rd)
    return lax.dot_general(a, b, (dims, ((), ())), preferred_element_type=jnp.float32)


def strip(refs, taps, lanes, j, out):
    length = refs[1].shape[0]
    count = taps.shape[0]
    at = pl.ds(pl.multiple_of(j * 8, 8), 8)
    for block in range(length // 8):
        acc = [None] * 8
        held = {}
        for k in range(count + 7):
            row = block * 8 + k
            value = refs[row // length][row % length, at, :]
            if k < count:
                held[k] = jnp.broadcast_to(taps[k : k + 1, lanes], value.shape)
            for i in range(8):
                t = k - i
                if 0 <= t < count:
                    term = held[t] * value
                    acc[i] = term if acc[i] is None else acc[i] + term
        out[0:8, block * 8 : block * 8 + 8, :] = jnp.swapaxes(jnp.stack(acc), 0, 1)


def lanes_of(half, own):
    return slice(half * own.shape[2], (half + 1) * own.shape[2])


def beam_kernel(half, low, own, high, taps, out):
    def one(j, _):
        strip((low, own, high), taps, lanes_of(half, own), j, out.at[j])

    lax.fori_loop(0, own.shape[1] // 8, one, None)


def beam(low, own, high, taps, half):
    a, b, f = own.shape
    assert taps.shape[0] == 2 * a + 1
    kernel = functools.partial(beam_kernel, half)
    return call(kernel, [(b // 8, 8, a, f)], low, own, high, taps, name="beam")[0]


def parted_kernel(half, k, parts, place, low, own, high, taps, loads, out):
    length = own.shape[0]
    lanes = lanes_of(half, own)
    strip((low, own, high), taps, lanes, lax.rem(place[1] + k, parts), out)
    for e in range(out.shape[0] - 8):
        out[8 + e] = loads[e * length : (e + 1) * length, lanes]


def parted_beam(place, low, own, high, taps, half, loads, k, parts):
    a, b, f = own.shape
    assert taps.shape[0] == 2 * a + 1 and b == 8 * parts
    shape = (8 + loads.shape[0] // a, a, f)
    kernel = functools.partial(parted_kernel, half, k, parts)
    return call(kernel, [shape], place, low, own, high, taps, loads, name="beam")[0].reshape(-1, f)


def source(place, k, parts):
    return lax.rem(place[1] + parts - k, parts)


def row_block(place, c, k, parts):
    return lax.rem(place[0] + c, 2) * parts + lax.rem(place[1] + k, parts)


def moment_kernel(c, pixels, place, *refs):
    if len(refs) > 3:
        out, hi, lo = refs[-3:]
        parts = hi.shape[0] // 2
        for s in range(2 * parts):
            value = refs[s][0:pixels]
            top = value.astype(jnp.bfloat16)
            b = 2 * source(place, s % parts, parts) + s // parts
            hi[b] = top
            lo[b] = (value - top.astype(jnp.float32)).astype(jnp.bfloat16)
    else:
        hi, lo, out = refs
        parts = hi.shape[0] // 2
    blocks = 2 * parts
    width = hi.shape[2]
    half = width // 2
    dims = (((0,), (0,)), ((), ()))
    upper = lax.rem(place[0] + c, 2) == 0
    for k in range(parts):
        i = row_block(place, c, k, parts)
        at = [lax.rem(i + j, blocks) for j in range(parts)]
        left = jnp.concatenate([lo[i], lo[i], hi[i], hi[i]], axis=0)
        high = jnp.concatenate([hi[b] for b in at], axis=1)
        low = jnp.concatenate([lo[b] for b in at], axis=1)
        right = jnp.concatenate([low, high, low, high], axis=0)
        block = lax.dot_general(left, right, dims, preferred_element_type=jnp.float32)
        for j in range(parts):
            out[k, j * width : (j + 1) * width, :] = block[:, j * width : (j + 1) * width]
        m = lax.rem(i, parts)
        left = jnp.concatenate([lo[m], lo[m], hi[m], hi[m]], axis=0)
        left = jnp.where(upper, left[:, :half], left[:, half:])
        m = m + parts
        right = jnp.concatenate([lo[m], hi[m], lo[m], hi[m]], axis=0)
        out[k, parts * width :, :] = lax.dot_general(
            left, right, dims, preferred_element_type=jnp.float32
        )


def moments(place, slots, pixels):
    width = slots[0].shape[1]
    parts = len(slots) // 2
    shape = (parts, width * parts + width // 2, width)
    halves = (2 * parts, pixels, width)
    half = jnp.bfloat16
    theirs, hi, lo = call(
        functools.partial(moment_kernel, 1, pixels), [shape, halves, halves], place, *slots,
        name="moments", dtypes=[jnp.float32, half, half],
    )
    ours = call(functools.partial(moment_kernel, 0, pixels), [shape], place, hi, lo, name="moments")
    return theirs, ours[0], hi, lo


def every(tile, r):
    return jnp.broadcast_to(tile[r : r + 1], tile.shape)


def along(tile, k):
    return jnp.broadcast_to(tile[:, k : k + 1], tile.shape)


def inverse_spd(matrix):
    n = matrix.shape[0]
    lane = lax.broadcasted_iota(jnp.int32, (8, n), 1)
    row = lax.broadcasted_iota(jnp.int32, (8, n), 0)
    tiles = [matrix[i : i + 8] for i in range(0, n, 8)]
    for p in range(n // 8):
        cols = [[along(t, 8 * p + j) for t in tiles] for j in range(8)]
        for r in range(8):
            k = 8 * p + r
            top = every(tiles[p], r)
            heads = [
                along(top, 8 * p + j) if r == 0 else every(cols[j][p], r) for j in range(r, 8)
            ]
            pivot = 1.0 / heads[0]
            first = jnp.where(lane == k, 1.0, top) * pivot
            left = cols[r]
            for j in range(r + 1, 8):
                factor = heads[j - r] * pivot
                cols[j] = [t - x * factor for t, x in zip(cols[j], left)]
                cols[j][p] = jnp.where(row == r, factor, cols[j][p])
            tiles = [jnp.where(lane == k, 0.0, t) - x * first for t, x in zip(tiles, left)]
            tiles[p] = jnp.where(row == r, first, tiles[p])
    return jnp.concatenate(tiles, axis=0)


def total(x):
    return jnp.sum(jnp.sum(x, axis=1, keepdims=True), axis=0, keepdims=True)


def identity(n):
    return lax.broadcasted_iota(jnp.int32, (n, n), 0) == lax.broadcasted_iota(jnp.int32, (n, n), 1)


def parts_of(x):
    return jnp.concatenate(split3(x), axis=0)


def gram_of(left, right):
    n = left.shape[0] // 3
    grid = lax.dot_general(
        left, right, (((1,), (1,)), ((), ())), preferred_element_type=jnp.float32
    )
    rows = grid[:n] + (grid[n : 2 * n] + grid[2 * n :])
    return rows[:, :n] + (rows[:, n : 2 * n] + rows[:, 2 * n :])


def times(matrix, right):
    n = matrix.shape[0]
    top, mid, low = split3(matrix)
    left = jnp.concatenate([low, mid, top, mid, top, top], axis=1)
    right = jnp.concatenate([right, right[: 2 * n], right[:n]], axis=0)
    return jnp.dot(left, right, preferred_element_type=jnp.float32)


def weights(pieces, gram, noise):
    inverse = inverse_spd(gram + jnp.where(identity(gram.shape[0]), noise, 0.0))
    return inverse, times(inverse, pieces)


def first_kernel(place, *refs):
    slots, (inverse_out, weight_out, loads) = refs[:-3], refs[-3:]
    parts = len(slots) // 2
    n = weight_out.shape[0]
    rows, width = slots[0].shape
    for s, ref in enumerate(slots):
        b = 2 * source(place, s % parts, parts) + s // parts
        loads[:, pl.ds(pl.multiple_of(b * width, width), width)] = ref[rows - n : rows]
    pieces = parts_of(loads[...])
    gram = gram_of(pieces, pieces)
    inverse_out[...], weight_out[...] = weights(pieces, gram, jnp.ones((1, 1), jnp.float32))


def first_weights(place, slots, n):
    shape = (n, len(slots) * slots[0].shape[1])
    scratch = [VM(shape, jnp.float32)]
    return call(first_kernel, [(n, n), shape], place, *slots, name="first", scratch=scratch)


def cross_of(stacked, hi, mid, low):
    n = stacked.shape[0] // 3

    def product(count, ref):
        return jnp.dot(stacked[: count * n], ref[...], preferred_element_type=jnp.float32)

    top, middle, last = product(3, hi), product(2, mid), product(1, low)
    small = top[2 * n :] + middle[n:] + last
    return top[:n] + (top[n : 2 * n] + middle[:n] + small)


def fit_kernel(pixel_total, parts, place, *refs):
    slots = refs[: 2 * parts]
    inverse0, weight0, map_hi, map_lo = refs[2 * parts : 2 * parts + 4]
    block_out, noise_out, lat_out, hi, mid, low, held = refs[2 * parts + 4 :]
    width = slots[0].shape[1]
    blocks = 2 * parts
    freqs = blocks * width
    n = weight0.shape[0]
    diagonal = identity(width)
    power = jnp.zeros((width, width), jnp.float32)

    def place_block(i, j, block, mirror):
        rows = pl.ds(pl.multiple_of(i * width, width), width)
        cols = pl.ds(pl.multiple_of(j * width, width), width)
        hi[rows, cols], mid[rows, cols], low[rows, cols] = split3(block)
        if mirror:
            hi[cols, rows], mid[cols, rows], low[cols, rows] = split3(block.T)

    for s, ref in enumerate(slots):
        i = row_block(place, s // parts, parts - s % parts, parts)
        for j in range(parts):
            place_block(i, lax.rem(i + j, blocks), ref[j * width : (j + 1) * width], j > 0)
        power = power + jnp.where(diagonal, ref[:width], 0.0)
    upper = place[0] == 0
    for k in range(parts):
        m = lax.rem(place[1] + parts - k, parts)
        ours, theirs = slots[k][parts * width :], slots[parts + k][parts * width :]
        block = jnp.concatenate(
            [jnp.where(upper, ours, theirs), jnp.where(upper, theirs, ours)], axis=0
        )
        place_block(m, m + parts, block, True)
    power = total(power)

    def step(_, state):
        inverse, weight, noise = state
        stacked = parts_of(weight)
        cross = cross_of(stacked, hi, mid, low)
        pieces = parts_of(cross)
        scaled = pixel_total * noise * inverse + gram_of(pieces, stacked)
        updated = times(inverse_spd(scaled), pieces)
        held[...] = updated
        pieces = parts_of(updated)
        gram = gram_of(pieces, pieces)
        noise = (power - 2.0 * total(updated * cross) + total(scaled * gram)) / (
            pixel_total * freqs
        )
        return (*weights(pieces, gram, noise), noise)

    state = (inverse0[...], weight0[...], jnp.ones((1, 1), jnp.float32))
    _, weight, noise = lax.fori_loop(0, ITERS, step, state)
    noise_out[...] = noise
    here = block_out.shape[1]
    block_out[...] = held[:, pl.ds(pl.multiple_of(place[1] * here, here), here)]
    whigh, wlow, _ = split3(weight)
    pair = jnp.concatenate([whigh, wlow], axis=0)
    latent = None
    for b in range(blocks):
        lanes = slice(b * width, (b + 1) * width)
        dims = (((1,), (1,)), ((), ()))
        both = lax.dot_general(
            pair[:, lanes], map_hi[b], dims, preferred_element_type=jnp.float32
        )
        term = lax.dot_general(
            whigh[:, lanes], map_lo[b], dims, preferred_element_type=jnp.float32
        )
        term = both[:n] + (both[n:] + term)
        latent = term if latent is None else latent + term
    lat_out[...] = latent


def fit(place, slots, inverse0, weight0, hi, lo, pixel_total):
    n, freqs = weight0.shape
    parts = hi.shape[0] // 2
    return call(
        functools.partial(fit_kernel, pixel_total, parts),
        [(n, freqs // parts), (1, 1), (n, hi.shape[1])],
        place, *slots, inverse0, weight0, hi, lo,
        name="fit",
        scratch=[VM((freqs, freqs), jnp.bfloat16)] * 3 + [VM((n, freqs), jnp.float32)],
    )


def clean_kernel(parts, place, *refs):
    latents, loads, slots = refs[:parts], refs[parts], refs[parts + 1 : 3 * parts + 1]
    out, held, sems = refs[3 * parts + 1 :]
    width = slots[0].shape[1]
    rows = latents[0].shape[1]
    copies = []
    for k in range(parts):
        model = thin(latents[k][...], loads[...], ((0,), (0,)))
        for h in range(2):
            lanes = slice(h * width, (h + 1) * width)
            held[k, :, lanes] = slots[h * parts + (parts - k) % parts][0:rows] - model[:, lanes]
        here = pl.ds(pl.multiple_of(source(place, k, parts) * rows, rows), rows)
        copies.append(pltpu.make_async_copy(held.at[k], out.at[here], sems.at[k]))
        copies[-1].start()
    for copy in copies:
        copy.wait()


def clean(place, slots, latents, loads):
    parts = len(latents)
    rows = latents[0].shape[1]
    wide = 2 * slots[0].shape[1]
    return call(
        functools.partial(clean_kernel, parts), [(parts * rows, wide)],
        place, *latents, loads, *slots,
        name="clean",
        scratch=[VM((parts, rows, wide), jnp.float32), pltpu.SemaphoreType.DMA((parts,))],
        out_space=pl.ANY,
    )[0]


def body(sky_maps, validity, row_taps, column_taps, init_loadings):
    rows_here, cols_here, freqs_here = sky_maps.shape
    sx, sy, af = (lax.axis_size(a) for a in ("sx", "sy", "af"))
    width = freqs_here // 2
    n = init_loadings.shape[1]
    pixels_here = rows_here * cols_here
    pixels = pixels_here // af
    place = jnp.stack([lax.rem(lax.axis_index("sx"), 2), lax.axis_index("af")]).astype(jnp.int32)
    mask = validity.astype(jnp.float32)[:, :, None]

    def halos(block, axis, count):
        low = lax.ppermute(block, axis, [(i, i + 1) for i in range(count - 1)])
        high = lax.ppermute(block, axis, [(i + 1, i) for i in range(count - 1)])
        return low, high

    def shifted(block, k):
        return lax.ppermute(block, "af", [(i, (i + k) % af) for i in range(af)])

    def swapped(block):
        return lax.ppermute(block, "sx", [(i, i ^ 1) for i in range(sx)])

    beamed, traded = [], []
    masked = [sky_maps[:, :, h * width : (h + 1) * width] * mask for h in range(2)]
    around = [halos(m, "sx", sx) for m in masked]
    for h in range(2):
        smoothed = beam(around[h][0], masked[h], around[h][1], row_taps.T, h)
        smoothed = smoothed.reshape(cols_here, rows_here, width)
        low, high = halos(smoothed, "sy", sy)
        slots, here = [None] * af, [None] * af
        for k in (*range(af // 2, af), *range(af // 2)):
            operands = (low, smoothed, high)
            slots[k] = parted_beam(
                place, *operands, column_taps.T, h, init_loadings.T, k, af
            )
            here[k] = shifted(slots[k], k) if k > 0 else slots[k]
        beamed += slots
        traded += here

    theirs, partial, hi, lo = moments(place, traded, pixels)
    partial = partial + swapped(theirs)
    inverse0, weight0 = first_weights(place, traded, n)
    piece = partial[0]
    for k in range(1, af):
        piece = piece + shifted(partial[k], k)
    piece, inverse0, weight0 = lax.optimization_barrier((piece, inverse0, weight0))
    ranks = sx * sy // 2
    groups = [[s * sy + t for s in range(c, sx, 2) for t in range(sy)] for c in range(2)]
    shape = piece.shape
    pieces = piece.reshape(-1, 2, shape[1])
    pieces = lax.all_to_all(
        pieces, ("sx", "sy"), 0, 0, axis_index_groups=groups, tiled=True
    )
    owned = jnp.sum(pieces.reshape(ranks, -1, 2, shape[1]), axis=0)
    pieces = jnp.broadcast_to(owned[None], (ranks, *owned.shape)).reshape(pieces.shape)
    pieces = lax.all_to_all(
        pieces, ("sx", "sy"), 0, 0, axis_index_groups=groups, tiled=True
    )
    piece = pieces.reshape(shape)
    mine = [piece] + [shifted(piece, k) for k in range(1, af)]
    other = [swapped(x) for x in mine]

    loads_here, noise, latent = fit(
        place, mine + other, inverse0, weight0, hi, lo, float(pixels_here * sx * sy)
    )
    latents = [latent] + [shifted(latent, k) for k in range(1, af)]
    cleaned = clean(place, beamed, latents, loads_here)
    return cleaned.reshape(rows_here, cols_here, freqs_here), loads_here.T, noise.reshape(())


def solution(mesh):
    placed = (P("sx", "sy", "af"), P("sx", "sy"), P("af", None), P("af", None), P("af", None))
    return jax.shard_map(
        body,
        mesh=mesh,
        in_specs=placed,
        out_specs=(P("sx", "sy", "af"), P("af", None), P()),
        check_vma=False,
    )
```

```python
import functools

import jax
import jax.numpy as jnp
from jax import lax
from jax.experimental import pallas as pl
from jax.experimental.pallas import tpu as pltpu
from jax.sharding import PartitionSpec as P

ITERS = 4
HI = lax.Precision.HIGHEST
VM = pltpu.VMEM
INTERPRET = False
LIMIT = 32 << 20


def call(kernel, out_shapes, *args, name, scratch=(), dtypes=None, out_space=VM):
    dtypes = dtypes or [jnp.float32] * len(out_shapes)
    fast = pl.BlockSpec(memory_space=VM)
    specs = [
        pl.BlockSpec(memory_space=pltpu.SMEM) if x.dtype == jnp.int32 else fast for x in args
    ]
    if INTERPRET or out_space is not VM:
        outs = [jax.ShapeDtypeStruct(s, d) for s, d in zip(out_shapes, dtypes)]
    else:
        outs = [VM(s, d) for s, d in zip(out_shapes, dtypes)]
    if not INTERPRET:
        args = [
            x if x.dtype == jnp.int32 else pltpu.with_memory_space_constraint(x, VM) for x in args
        ]
    return pl.pallas_call(
        kernel,
        out_shape=outs,
        in_specs=specs,
        out_specs=[pl.BlockSpec(memory_space=out_space)] * len(outs),
        scratch_shapes=list(scratch),
        compiler_params=pltpu.CompilerParams(vmem_limit_bytes=LIMIT),
        interpret=INTERPRET,
        name=name,
    )(*args)


def contract(left, right, dims):
    return lax.dot_general(
        left, right, (dims, ((), ())), precision=HI, preferred_element_type=jnp.float32
    )


def split3(x):
    hi = x.astype(jnp.bfloat16)
    rest = x - hi.astype(jnp.float32)
    mid = rest.astype(jnp.bfloat16)
    low = (rest - mid.astype(jnp.float32)).astype(jnp.bfloat16)
    return hi, mid, low


def thin(left, right, dims):
    (ld,), (rd,) = dims
    lh, lm, ll = split3(left)
    rh, rm, rl = split3(right)
    a = jnp.concatenate([ll, lm, lh, lm, lh, lh], axis=ld)
    b = jnp.concatenate([rh, rm, rl, rh, rm, rh], axis=rd)
    return lax.dot_general(a, b, (dims, ((), ())), preferred_element_type=jnp.float32)


def strip(refs, taps, lanes, j, out):
    length = refs[1].shape[0]
    count = taps.shape[0]
    at = pl.ds(pl.multiple_of(j * 8, 8), 8)
    for block in range(length // 8):
        acc = [None] * 8
        held = {}
        for k in range(count + 7):
            row = block * 8 + k
            value = refs[row // length][row % length, at, :]
            if k < count:
                held[k] = jnp.broadcast_to(taps[k : k + 1, lanes], value.shape)
            for i in range(8):
                t = k - i
                if 0 <= t < count:
                    term = held[t] * value
                    acc[i] = term if acc[i] is None else acc[i] + term
        out[0:8, block * 8 : block * 8 + 8, :] = jnp.swapaxes(jnp.stack(acc), 0, 1)


def lanes_of(half, own):
    return slice(half * own.shape[2], (half + 1) * own.shape[2])


def beam_kernel(half, low, own, high, taps, out):
    def one(j, _):
        strip((low, own, high), taps, lanes_of(half, own), j, out.at[j])

    lax.fori_loop(0, own.shape[1] // 8, one, None)


def beam(low, own, high, taps, half):
    a, b, f = own.shape
    assert taps.shape[0] == 2 * a + 1
    kernel = functools.partial(beam_kernel, half)
    return call(kernel, [(b // 8, 8, a, f)], low, own, high, taps, name="beam")[0]


def parted_kernel(half, k, parts, place, low, own, high, taps, loads, out):
    length = own.shape[0]
    lanes = lanes_of(half, own)
    strip((low, own, high), taps, lanes, lax.rem(place[1] + k, parts), out)
    for e in range(out.shape[0] - 8):
        out[8 + e] = loads[e * length : (e + 1) * length, lanes]


def parted_beam(place, low, own, high, taps, half, loads, k, parts):
    a, b, f = own.shape
    assert taps.shape[0] == 2 * a + 1 and b == 8 * parts
    shape = (8 + loads.shape[0] // a, a, f)
    kernel = functools.partial(parted_kernel, half, k, parts)
    return call(kernel, [shape], place, low, own, high, taps, loads, name="beam")[0].reshape(-1, f)


def source(place, k, parts):
    return lax.rem(place[1] + parts - k, parts)


def row_block(place, c, k, parts):
    return lax.rem(place[0] + c, 2) * parts + lax.rem(place[1] + k, parts)


def moment_kernel(c, pixels, place, *refs):
    if len(refs) > 3:
        out, hi, lo = refs[-3:]
        parts = hi.shape[0] // 2
        for s in range(2 * parts):
            value = refs[s][0:pixels]
            top = value.astype(jnp.bfloat16)
            b = 2 * source(place, s % parts, parts) + s // parts
            hi[b] = top
            lo[b] = (value - top.astype(jnp.float32)).astype(jnp.bfloat16)
    else:
        hi, lo, out = refs
        parts = hi.shape[0] // 2
    blocks = 2 * parts
    width = hi.shape[2]
    half = width // 2
    dims = (((0,), (0,)), ((), ()))
    upper = lax.rem(place[0] + c, 2) == 0
    for k in range(parts):
        i = row_block(place, c, k, parts)
        at = [lax.rem(i + j, blocks) for j in range(parts)]
        left = jnp.concatenate([lo[i], lo[i], hi[i], hi[i]], axis=0)
        high = jnp.concatenate([hi[b] for b in at], axis=1)
        low = jnp.concatenate([lo[b] for b in at], axis=1)
        right = jnp.concatenate([low, high, low, high], axis=0)
        block = lax.dot_general(left, right, dims, preferred_element_type=jnp.float32)
        for j in range(parts):
            out[k, j * width : (j + 1) * width, :] = block[:, j * width : (j + 1) * width]
        m = lax.rem(i, parts)
        left = jnp.concatenate([lo[m], lo[m], hi[m], hi[m]], axis=0)
        left = jnp.where(upper, left[:, :half], left[:, half:])
        m = m + parts
        right = jnp.concatenate([lo[m], hi[m], lo[m], hi[m]], axis=0)
        out[k, parts * width :, :] = lax.dot_general(
            left, right, dims, preferred_element_type=jnp.float32
        )


def moments(place, slots, pixels):
    width = slots[0].shape[1]
    parts = len(slots) // 2
    shape = (parts, width * parts + width // 2, width)
    halves = (2 * parts, pixels, width)
    half = jnp.bfloat16
    theirs, hi, lo = call(
        functools.partial(moment_kernel, 1, pixels), [shape, halves, halves], place, *slots,
        name="moments", dtypes=[jnp.float32, half, half],
    )
    ours = call(functools.partial(moment_kernel, 0, pixels), [shape], place, hi, lo, name="moments")
    return theirs, ours[0], hi, lo


def every(tile, r):
    return jnp.broadcast_to(tile[r : r + 1], tile.shape)


def along(tile, k):
    return jnp.broadcast_to(tile[:, k : k + 1], tile.shape)


def inverse_spd(matrix):
    n = matrix.shape[0]
    lane = lax.broadcasted_iota(jnp.int32, (8, n), 1)
    row = lax.broadcasted_iota(jnp.int32, (8, n), 0)
    tiles = [matrix[i : i + 8] for i in range(0, n, 8)]
    for p in range(n // 8):
        cols = [[along(t, 8 * p + j) for t in tiles] for j in range(8)]
        for r in range(8):
            k = 8 * p + r
            top = every(tiles[p], r)
            heads = [
                along(top, 8 * p + j) if r == 0 else every(cols[j][p], r) for j in range(r, 8)
            ]
            pivot = 1.0 / heads[0]
            first = jnp.where(lane == k, 1.0, top) * pivot
            left = cols[r]
            for j in range(r + 1, 8):
                factor = heads[j - r] * pivot
                cols[j] = [t - x * factor for t, x in zip(cols[j], left)]
                cols[j][p] = jnp.where(row == r, factor, cols[j][p])
            tiles = [jnp.where(lane == k, 0.0, t) - x * first for t, x in zip(tiles, left)]
            tiles[p] = jnp.where(row == r, first, tiles[p])
    return jnp.concatenate(tiles, axis=0)


def total(x):
    return jnp.sum(jnp.sum(x, axis=1, keepdims=True), axis=0, keepdims=True)


def identity(n):
    return lax.broadcasted_iota(jnp.int32, (n, n), 0) == lax.broadcasted_iota(jnp.int32, (n, n), 1)


def parts_of(x):
    return jnp.concatenate(split3(x), axis=0)


def gram_of(left, right):
    n = left.shape[0] // 3
    grid = lax.dot_general(
        left, right, (((1,), (1,)), ((), ())), preferred_element_type=jnp.float32
    )
    rows = grid[:n] + (grid[n : 2 * n] + grid[2 * n :])
    return rows[:, :n] + (rows[:, n : 2 * n] + rows[:, 2 * n :])


def times(matrix, right):
    n = matrix.shape[0]
    top, mid, low = split3(matrix)
    left = jnp.concatenate([low, mid, top, mid, top, top], axis=1)
    right = jnp.concatenate([right, right[: 2 * n], right[:n]], axis=0)
    return jnp.dot(left, right, preferred_element_type=jnp.float32)


def regularized(gram, noise):
    return inverse_spd(gram + jnp.where(identity(gram.shape[0]), noise, 0.0))


def cross_of(stacked, hi, mid, low):
    n = stacked.shape[0] // 3

    def product(count, ref):
        return jnp.dot(stacked[: count * n], ref[...], preferred_element_type=jnp.float32)

    top, middle, last = product(3, hi), product(2, mid), product(1, low)
    small = top[2 * n :] + middle[n:] + last
    return top[:n] + (top[n : 2 * n] + middle[:n] + small)


def fit_kernel(pixel_total, parts, place, *refs):
    slots, maps = refs[: 2 * parts], refs[2 * parts : 4 * parts]
    map_hi, map_lo = refs[4 * parts : 4 * parts + 2]
    block_out, noise_out, lat_out, hi, mid, low, held = refs[4 * parts + 2 :]
    width = slots[0].shape[1]
    blocks = 2 * parts
    freqs = blocks * width
    n = held.shape[0]
    diagonal = identity(width)
    power = jnp.zeros((width, width), jnp.float32)

    def place_block(i, j, block, mirror):
        rows = pl.ds(pl.multiple_of(i * width, width), width)
        cols = pl.ds(pl.multiple_of(j * width, width), width)
        hi[rows, cols], mid[rows, cols], low[rows, cols] = split3(block)
        if mirror:
            hi[cols, rows], mid[cols, rows], low[cols, rows] = split3(block.T)

    for s, ref in enumerate(slots):
        i = row_block(place, s // parts, parts - s % parts, parts)
        for j in range(parts):
            place_block(i, lax.rem(i + j, blocks), ref[j * width : (j + 1) * width], j > 0)
        power = power + jnp.where(diagonal, ref[:width], 0.0)
    upper = place[0] == 0
    for k in range(parts):
        m = lax.rem(place[1] + parts - k, parts)
        ours, theirs = slots[k][parts * width :], slots[parts + k][parts * width :]
        block = jnp.concatenate(
            [jnp.where(upper, ours, theirs), jnp.where(upper, theirs, ours)], axis=0
        )
        place_block(m, m + parts, block, True)
    power = total(power)

    for p, ref in enumerate(maps):
        b = 2 * source(place, p % parts, parts) + p // parts
        rows = ref.shape[0]
        held[:, pl.ds(pl.multiple_of(b * width, width), width)] = ref[rows - n : rows]

    def step(_, state):
        gram, noise = state
        pieces = parts_of(held[...])
        raw = cross_of(pieces, hi, mid, low)
        inverse = regularized(gram, noise)
        weight = parts_of(times(inverse, pieces))
        cross = times(inverse, parts_of(raw))
        pieces = parts_of(cross)
        scaled = pixel_total * noise * inverse + gram_of(pieces, weight)
        updated = times(inverse_spd(scaled), pieces)
        held[...] = updated
        pieces = parts_of(updated)
        gram = gram_of(pieces, pieces)
        noise = (power - 2.0 * total(updated * cross) + total(scaled * gram)) / (
            pixel_total * freqs
        )
        return gram, noise

    pieces = parts_of(held[...])
    state = (gram_of(pieces, pieces), jnp.ones((1, 1), jnp.float32))
    gram, noise = lax.fori_loop(0, ITERS, step, state)
    weight = times(regularized(gram, noise), parts_of(held[...]))
    noise_out[...] = noise
    here = block_out.shape[1]
    block_out[...] = held[:, pl.ds(pl.multiple_of(place[1] * here, here), here)]
    whigh, wlow, _ = split3(weight)
    pair = jnp.concatenate([whigh, wlow], axis=0)
    latent = None
    for b in range(blocks):
        lanes = slice(b * width, (b + 1) * width)
        dims = (((1,), (1,)), ((), ()))
        both = lax.dot_general(
            pair[:, lanes], map_hi[b], dims, preferred_element_type=jnp.float32
        )
        term = lax.dot_general(
            whigh[:, lanes], map_lo[b], dims, preferred_element_type=jnp.float32
        )
        term = both[:n] + (both[n:] + term)
        latent = term if latent is None else latent + term
    lat_out[...] = latent


def fit(place, slots, maps, hi, lo, n, pixel_total):
    blocks, pixels, width = hi.shape
    freqs = blocks * width
    return call(
        functools.partial(fit_kernel, pixel_total, blocks // 2),
        [(n, 2 * width), (1, 1), (n, pixels)],
        place, *slots, *maps, hi, lo,
        name="fit",
        scratch=[VM((freqs, freqs), jnp.bfloat16)] * 3 + [VM((n, freqs), jnp.float32)],
    )


def clean_kernel(parts, place, *refs):
    latents, loads, slots = refs[:parts], refs[parts], refs[parts + 1 : 3 * parts + 1]
    out, held, sems = refs[3 * parts + 1 :]
    width = slots[0].shape[1]
    rows = latents[0].shape[1]
    copies = []
    for k in range(parts):
        model = thin(latents[k][...], loads[...], ((0,), (0,)))
        for h in range(2):
            lanes = slice(h * width, (h + 1) * width)
            held[k, :, lanes] = slots[h * parts + (parts - k) % parts][0:rows] - model[:, lanes]
        here = pl.ds(pl.multiple_of(source(place, k, parts) * rows, rows), rows)
        copies.append(pltpu.make_async_copy(held.at[k], out.at[here], sems.at[k]))
        copies[-1].start()
    for copy in copies:
        copy.wait()


def clean(place, slots, latents, loads):
    parts = len(latents)
    rows = latents[0].shape[1]
    wide = 2 * slots[0].shape[1]
    return call(
        functools.partial(clean_kernel, parts), [(parts * rows, wide)],
        place, *latents, loads, *slots,
        name="clean",
        scratch=[VM((parts, rows, wide), jnp.float32), pltpu.SemaphoreType.DMA((parts,))],
        out_space=pl.ANY,
    )[0]


def body(sky_maps, validity, row_taps, column_taps, init_loadings):
    rows_here, cols_here, freqs_here = sky_maps.shape
    sx, sy, af = (lax.axis_size(a) for a in ("sx", "sy", "af"))
    width = freqs_here // 2
    n = init_loadings.shape[1]
    pixels_here = rows_here * cols_here
    pixels = pixels_here // af
    place = jnp.stack([lax.rem(lax.axis_index("sx"), 2), lax.axis_index("af")]).astype(jnp.int32)
    mask = validity.astype(jnp.float32)[:, :, None]

    def halos(block, axis, count):
        low = lax.ppermute(block, axis, [(i, i + 1) for i in range(count - 1)])
        high = lax.ppermute(block, axis, [(i + 1, i) for i in range(count - 1)])
        return low, high

    def shifted(block, k):
        return lax.ppermute(block, "af", [(i, (i + k) % af) for i in range(af)])

    def swapped(block):
        return lax.ppermute(block, "sx", [(i, i ^ 1) for i in range(sx)])

    beamed, traded = [], []
    masked = [sky_maps[:, :, h * width : (h + 1) * width] * mask for h in range(2)]
    around = [halos(m, "sx", sx) for m in masked]
    for h in range(2):
        smoothed = beam(around[h][0], masked[h], around[h][1], row_taps.T, h)
        smoothed = smoothed.reshape(cols_here, rows_here, width)
        low, high = halos(smoothed, "sy", sy)
        slots, here = [None] * af, [None] * af
        for k in (*range(af // 2, af), *range(af // 2)):
            operands = (low, smoothed, high)
            slots[k] = parted_beam(
                place, *operands, column_taps.T, h, init_loadings.T, k, af
            )
            here[k] = shifted(slots[k], k) if k > 0 else slots[k]
        beamed += slots
        traded += here

    theirs, partial, hi, lo = moments(place, traded, pixels)
    partial = partial + swapped(theirs)
    piece = partial[0]
    for k in range(1, af):
        piece = piece + shifted(partial[k], k)
    ranks = sx * sy // 2
    groups = [[s * sy + t for s in range(c, sx, 2) for t in range(sy)] for c in range(2)]
    shape = piece.shape
    pieces = piece.reshape(-1, 2, shape[1])
    pieces = lax.all_to_all(
        pieces, ("sx", "sy"), 0, 0, axis_index_groups=groups, tiled=True
    )
    owned = jnp.sum(pieces.reshape(ranks, -1, 2, shape[1]), axis=0)
    pieces = jnp.broadcast_to(owned[None], (ranks, *owned.shape)).reshape(pieces.shape)
    pieces = lax.all_to_all(
        pieces, ("sx", "sy"), 0, 0, axis_index_groups=groups, tiled=True
    )
    piece = pieces.reshape(shape)
    mine = [piece] + [shifted(piece, k) for k in range(1, af)]
    other = [swapped(x) for x in mine]

    loads_here, noise, latent = fit(
        place, mine + other, traded, hi, lo, n, float(pixels_here * sx * sy)
    )
    latents = [latent] + [shifted(latent, k) for k in range(1, af)]
    cleaned = clean(place, beamed, latents, loads_here)
    return cleaned.reshape(rows_here, cols_here, freqs_here), loads_here.T, noise.reshape(())


def solution(mesh):
    placed = (P("sx", "sy", "af"), P("sx", "sy"), P("af", None), P("af", None), P("af", None))
    return jax.shard_map(
        body,
        mesh=mesh,
        in_specs=placed,
        out_specs=(P("sx", "sy", "af"), P("af", None), P()),
        check_vma=False,
    )
```
